32 devices in a mesh: gx: 4 (over y, x), gy: 2 (over core), gz: 4 (over z).
Axes of the slice: x: 2, y: 2, z: 4, core: 2. Of those that a mesh axis runs over, the one named last changes fastest.
Arguments:
- dual_operators: bfloat16 [4, 2, 4, 768, 768], P('gx', 'gy', 'gz'), may hold values from -1 to 3, as said below
- dual_load: float32 [4, 2, 4, 32, 384], P('gx', 'gy', 'gz'), may hold values from -25 to 25
- rigid_modes: float32 [4, 2, 4, 6, 768], P('gx', 'gy', 'gz'), may hold values from -0.21875 to 0.21875
- coarse_load: float32 [4, 2, 4, 6, 32], P('gx', 'gy', 'gz'), may hold values from -24 to 24
- mode_counts: int32 [4, 2, 4], P('gx', 'gy', 'gz'), may hold values from 3 to 6
- face_maps: int32 [4, 2, 4, 3, 128], P('gx', 'gy', 'gz'), may hold values from 0 to 127, each once within a row
Outputs:
- multipliers: float32 [4, 2, 4, 32, 384], P('gx', 'gy', 'gz')
- residual: float32 [4, 2, 4, 32, 384], P('gx', 'gy', 'gz')
The draws below stay inside these ranges and needn't reach their ends.
Inputs may be any that keep to these rules, and one draw needn't show every extreme that they name: Each dual_operators[i, j, k] is symmetric positive definite. Subdomain s uses rows 0 to mode_counts[s] - 1 of rigid_modes[s]. Each face_maps[i, j, k, d] holds every number of 0 to 127 once.
All inputs are finite; a program needn't handle non-finite values.
Results may differ from the reference program's by a relative error of at most 0.012.
Values sent between devices are 32-bit elements; how exact they have to be, the bound alone decides.
A program may use at most 64 MiB of HBM per device.

```python
import math
import jax
import jax.numpy as jnp
from jax import lax

IDOF = 768
FACE = 128
RHS = 32
MODES = 6
ITERS = 2
NSX = 4
NSY = 2
NSZ = 4


def draw_dual_operators(key, part):
    spread = 0.7 / math.sqrt(2.0 * IDOF)
    identity = jnp.eye(IDOF, dtype=jnp.float32)

    def one_column(position):
        column_key = jax.random.fold_in(key, position)
        noise_key = jax.random.fold_in(column_key, 1)
        scale_key = jax.random.fold_in(column_key, 2)
        noise_part = jax.random.truncated_normal(noise_key, -4.0, 4.0, (NSZ, IDOF, IDOF), jnp.float32) * spread
        coupling = identity + 0.5 * (noise_part + jnp.swapaxes(noise_part, 1, 2))
        diagonal = jnp.exp(jax.random.uniform(scale_key, (NSZ, IDOF), jnp.float32, math.log(0.25), math.log(2.0)))
        root_scale = jnp.sqrt(diagonal)
        outer_scale = root_scale[:, :, None] * root_scale[:, None, :]
        return (coupling * outer_scale).astype(jnp.bfloat16)
    blocks = lax.map(one_column, jnp.arange(NSX * NSY))
    return blocks.reshape(NSX, NSY, NSZ, IDOF, IDOF)


def draw_dual_load(key, part):
    grid_key = jax.random.fold_in(key, 11)
    column_key = jax.random.fold_in(key, 12)
    value_key = jax.random.fold_in(key, 13)
    location = (jnp.arange(NSX)[:, None, None] + jnp.arange(NSY)[None, :, None] + jnp.arange(NSZ)[None, None, :]).astype(jnp.float32) / (NSX + NSY + NSZ - 3)
    rising = (1.0 + 2.0 * location) / math.sqrt(3.0)
    subdomain_scale = jnp.exp(jax.random.uniform(grid_key, (NSX, NSY, NSZ), jnp.float32, math.log(0.1), math.log(1.0)))
    column_scale = jnp.exp(jax.random.uniform(column_key, (RHS,), jnp.float32, math.log(0.3), math.log(3.0)))
    full_shape = (NSX, NSY, NSZ, RHS, 3 * FACE)
    values = jax.random.truncated_normal(value_key, -4.0, 4.0, full_shape, jnp.float32)
    scales = (rising * subdomain_scale)[:, :, :, None, None] * column_scale[None, None, None, :, None]
    return values * scales


def set_ends(drawn, own_key, low, high):
    shape = drawn.shape
    index_at = [jax.random.randint(jax.random.fold_in(own_key, axis), (), 0, shape[axis]) for axis in range(len(shape))]
    drawn = drawn.at[tuple(index_at)].set(low)
    longest = shape.index(max(shape))
    index_at[longest] = (index_at[longest] + 1) % shape[longest]
    return drawn.at[tuple(index_at)].set(high)


def shard_levels(own_key, dims, split, smallest, largest):
    gain = 1.0
    for dim, shards_of in split:
        heights = jax.random.uniform(jax.random.fold_in(jax.random.fold_in(own_key, 6), dim), (shards_of,), jnp.float32, smallest / len(split), largest / len(split))
        gain = gain * jnp.repeat(jnp.exp(heights), dims[dim] // shards_of).reshape((-1,) + (1,) * (len(dims) - 1 - dim))
    return gain


def gaussian(own_key, dims, width, bound, cuts=(), kind=jnp.bfloat16):
    loudness = shard_levels(own_key, dims, cuts, -0.22, 0.18) if cuts else 1.0
    array = jax.random.normal(own_key, dims, jnp.float32) * width * loudness
    return jnp.minimum(jnp.maximum(array, -bound), bound).astype(kind)


def setup_inputs(seed: int = 0) -> dict:
    arg_keys = jax.random.split(jax.random.key(seed), 7)
    dual_operators = draw_dual_operators(jax.random.fold_in(arg_keys[6], 71), 0)
    dual_load = draw_dual_load(jax.random.fold_in(arg_keys[6], 71), 0)
    rigid_modes = gaussian(arg_keys[2], (NSX, NSY, NSZ, MODES, IDOF), IDOF ** -0.5, 0.21875, ((0, 4), (1, 2), (2, 4)), jnp.float32)
    coarse_load = gaussian(arg_keys[3], (NSX, NSY, NSZ, MODES, RHS), 4.0, 24.0, ((0, 4), (1, 2), (2, 4)), jnp.float32)
    mode_counts = set_ends(jax.random.randint(arg_keys[4], (NSX, NSY, NSZ), 3, MODES + 1), jax.random.fold_in(arg_keys[4], 1), 3, MODES).astype(jnp.int32)
    face_maps = jax.vmap(lambda own: jax.random.permutation(own, FACE))(jax.random.split(arg_keys[5], NSX * NSY * NSZ * 3)).reshape((NSX, NSY, NSZ, 3, FACE)).astype(jnp.int32)
    return dict(dual_operators=dual_operators, dual_load=dual_load, rigid_modes=rigid_modes, coarse_load=coarse_load, mode_counts=mode_counts, face_maps=face_maps)


def reorder(values, face_order):
    index_table = jnp.broadcast_to(face_order[..., None, :], values.shape)
    return jnp.take_along_axis(values, index_table, axis=-1)

def side_flags(position, extent):
    return jnp.stack([position > 0, position < extent - 1], axis=-1).astype(jnp.float32)

def interface_mask(first_flags, second_flags, third_flags, face_width):
    grid_shape = (first_flags.shape[0], second_flags.shape[0], third_flags.shape[0], 2)
    present = jnp.concatenate([jnp.broadcast_to(first_flags[:, None, None, :], grid_shape), jnp.broadcast_to(second_flags[None, :, None, :], grid_shape), jnp.broadcast_to(third_flags[None, None, :, :], grid_shape)], axis=-1)
    return jnp.repeat(present, face_width, axis=-1)[:, :, :, None, :]

def face_block(values, face_index, face_width):
    return values[..., face_index * face_width:(face_index + 1) * face_width]

def from_lower(block, spatial):
    length = block.shape[spatial]
    padding = jnp.zeros_like(lax.slice_in_dim(block, 0, 1, axis=spatial))
    return jnp.concatenate([padding, lax.slice_in_dim(block, 0, length - 1, axis=spatial)], axis=spatial)

def from_upper(block, spatial):
    length = block.shape[spatial]
    padding = jnp.zeros_like(lax.slice_in_dim(block, 0, 1, axis=spatial))
    return jnp.concatenate([lax.slice_in_dim(block, 1, length, axis=spatial), padding], axis=spatial)

def assemble(local_values, face_maps, inverse, present):
    pieces = []
    for spatial in range(3):
        minus_face = face_block(local_values, 2 * spatial, FACE)
        plus_face = face_block(local_values, 2 * spatial + 1, FACE)
        owner_minus = reorder(minus_face, inverse[:, :, :, spatial, :])
        pieces.append(minus_face - reorder(from_lower(plus_face, spatial), face_maps[:, :, :, spatial, :]))
        pieces.append(plus_face - from_upper(owner_minus, spatial))
    return jnp.concatenate(pieces, axis=-1) * present

def apply_dual(local_values, dual_operators, face_maps, inverse, present):
    rounded = local_values.astype(jnp.bfloat16)

    def one_slab(operands):
        slab_operators, slab_values = operands
        return jnp.einsum('yzrk,yzki->yzri', slab_values.astype(jnp.float32), slab_operators.astype(jnp.float32), precision=lax.Precision.HIGHEST)
    products = lax.map(one_slab, (dual_operators, rounded))
    return assemble(products, face_maps, inverse, present)

def coarse_factor(mode_rows, active):
    identity = jnp.eye(active.shape[-1], dtype=jnp.float32)
    normal_matrix = jnp.einsum('xyzmi,xyzni->xyzmn', mode_rows, mode_rows, precision=lax.Precision.HIGHEST)
    normal_matrix = normal_matrix + identity * (1.0 - active)[..., None, :]
    factor = jnp.linalg.cholesky(normal_matrix)
    return jax.scipy.linalg.cho_solve((factor, True), jnp.broadcast_to(identity, normal_matrix.shape))

def spread_coarse(coefficients, mode_rows):
    return jnp.einsum('xyzmr,xyzmi->xyzri', coefficients, mode_rows, precision=lax.Precision.HIGHEST)

def owned_faces(values):
    return jnp.concatenate([face_block(values, 1, FACE), face_block(values, 3, FACE), face_block(values, 5, FACE)], axis=-1)

def pairing(first_vectors, second_vectors):
    return jnp.einsum('xyzri,xyzsi->rs', owned_faces(first_vectors), owned_faces(second_vectors), precision=lax.Precision.HIGHEST)

def combine_columns(vectors, matrix):
    return jnp.einsum('xyzri,rs->xyzsi', vectors, matrix, precision=lax.Precision.HIGHEST)

def cholesky_solve(matrix, right_side):
    factor = jnp.linalg.cholesky(matrix)
    return jax.scipy.linalg.cho_solve((factor, True), right_side)

def reference(dual_operators, dual_load, rigid_modes, coarse_load, mode_counts, face_maps):
    present = interface_mask(side_flags(jnp.arange(NSX), NSX), side_flags(jnp.arange(NSY), NSY), side_flags(jnp.arange(NSZ), NSZ), FACE)
    inverse = jnp.argsort(face_maps, axis=-1).astype(jnp.int32)
    active = (jnp.arange(MODES)[None, None, None, :] < mode_counts[..., None]).astype(jnp.float32)
    mode_rows = rigid_modes * present * active[..., None]
    coarse_inverse = coarse_factor(mode_rows, active)

    def coarse_field(coefficients):
        return assemble(spread_coarse(coefficients, mode_rows), face_maps, inverse, present)

    def precondition(current):
        weights = jnp.einsum('xyzmi,xyzri->xyzmr', mode_rows, current, precision=lax.Precision.HIGHEST)
        coefficients = jnp.einsum('xyzmn,xyznr->xyzmr', coarse_inverse, weights, precision=lax.Precision.HIGHEST)
        return current - 0.25 * coarse_field(coefficients)

    def operator(current):
        return apply_dual(current, dual_operators, face_maps, inverse, present)
    empty_face = jnp.zeros_like(dual_load[..., :FACE])
    spread_load = jnp.concatenate([empty_face, dual_load[..., :FACE], empty_face, dual_load[..., FACE:2 * FACE], empty_face, dual_load[..., 2 * FACE:]], axis=-1)
    right_local = assemble(spread_load, face_maps, inverse, present)
    initial = coarse_field(jnp.einsum('xyzmn,xyznr->xyzmr', coarse_inverse, coarse_load * active[..., None], precision=lax.Precision.HIGHEST))
    multipliers = initial
    residual = right_local - operator(initial)
    direction = residual
    image = residual
    residual_gram = jnp.zeros((RHS, RHS), jnp.float32)
    for iteration in range(ITERS):
        projected = precondition(residual)
        projected_image = operator(projected)
        fresh_gram = pairing(projected, residual)
        if iteration == 0:
            direction = projected
            image = projected_image
        else:
            update_gram = cholesky_solve(residual_gram, fresh_gram)
            direction = projected + combine_columns(direction, update_gram)
            image = projected_image + combine_columns(image, update_gram)
        residual_gram = fresh_gram
        step_gram = cholesky_solve(pairing(direction, image), residual_gram)
        multipliers = multipliers + combine_columns(direction, step_gram)
        residual = residual - combine_columns(image, step_gram)
    return (owned_faces(multipliers), owned_faces(residual))
```

```python
import functools

import jax
import jax.numpy as jnp
from jax import lax
from jax.experimental import pallas as pl
from jax.experimental.pallas import tpu as pltpu
from jax.sharding import PartitionSpec as P

MESH = pl.DeviceIdType.MESH
HIGH = lax.Precision.HIGHEST
NN = (((1,), (0,)), ((), ()))
NT = (((1,), (1,)), ((), ()))
TN = (((0,), (0,)), ((), ()))


def mul(a, b, dims=NN):
    return lax.dot_general(a, b, dims, precision=HIGH, preferred_element_type=jnp.float32)


def eliminate(system, size):
    rows = lax.broadcasted_iota(jnp.int32, system.shape, 0)
    for k in range(size):
        row = system[k : k + 1, :]
        column = system[:, k : k + 1]
        scaled = row / row[:, k : k + 1]
        system = jnp.where(rows == k, scaled, system - column * scaled)
    return system[:, size:]


def identity(size):
    return (
        lax.broadcasted_iota(jnp.int32, (size, size), 0)
        == lax.broadcasted_iota(jnp.int32, (size, size), 1)
    ).astype(jnp.float32)


def packed(gram, width):
    groups = max(1, width // gram.shape[1])
    depth = gram.shape[0] // groups
    return jnp.concatenate([gram[g * depth : (g + 1) * depth] for g in range(groups)], axis=1)


def unpacked(tile, size):
    groups = max(1, tile.shape[1] // size)
    return jnp.concatenate([tile[:, g * size : (g + 1) * size] for g in range(groups)], axis=0)


def kernel(
    extents,
    operator_hbm,
    load_ref,
    modes_ref,
    coarse_ref,
    count_ref,
    maps_ref,
    multipliers_ref,
    residual_ref,
    raw,
    ordered,
    own_modes,
    minus_modes,
    all_modes,
    padded_load,
    coefficients,
    face_out,
    face_in,
    load_in,
    plane_sums,
    line_sums,
    raw_sem,
    coefficient_send,
    coefficient_recv,
    face_send,
    face_recv,
    mode_send,
    mode_recv,
    load_send,
    load_recv,
    plane_send,
    plane_recv,
    line_send,
    line_recv,
):
    nx, ny, nz = extents
    cases = load_ref.shape[0]
    width = load_ref.shape[1] // 3
    modes = modes_ref.shape[0]
    padded = own_modes.shape[0]
    here = (lax.axis_index("gx"), lax.axis_index("gy"), lax.axis_index("gz"))
    ix, iy, iz = here
    plane = nx * ny
    slot = ix * ny + iy

    fetch = pltpu.make_async_copy(operator_hbm, raw, raw_sem)
    fetch.start()

    for phase in range(3):
        coefficients[phase] = jnp.zeros(coefficients.shape[1:], jnp.float32)
    all_modes[...] = jnp.zeros(all_modes.shape, jnp.float32)
    own_modes[...] = jnp.zeros(own_modes.shape, jnp.float32)
    padded_load[...] = jnp.zeros(padded_load.shape, jnp.float32)

    def plane_peer(offset):
        other = lax.rem(slot + offset, plane)
        return (lax.div(other, ny), lax.rem(other, ny), iz)

    def line_peer(offset):
        return (ix, iy, lax.rem(iz + offset, nz))

    barrier = pltpu.get_barrier_semaphore()
    for offset in range(1, plane):
        pl.semaphore_signal(barrier, inc=1, device_id=plane_peer(offset), device_id_type=MESH)
    for offset in range(1, nz):
        pl.semaphore_signal(barrier, inc=1, device_id=line_peer(offset), device_id_type=MESH)

    exists = []
    neighbour = []
    for d in range(3):
        exists.append(here[d] > 0)
        exists.append(here[d] < extents[d] - 1)
        for step in (-1, 1):
            neighbour.append(tuple(here[a] + (step if a == d else 0) for a in range(3)))
    flags = [jnp.where(e, 1, 0).astype(jnp.int32) for e in exists]

    def face(values, f):
        return values[:, f * width : (f + 1) * width]

    def masked(values, f):
        return jnp.where(jnp.full(values.shape, flags[f], jnp.int32) == 1, values, 0.0)

    waits = []

    def remote(source, target, send, recv, where):
        return pltpu.make_async_remote_copy(
            src_ref=source,
            dst_ref=target,
            send_sem=send,
            recv_sem=recv,
            device_id=where,
            device_id_type=MESH,
        )

    def start_to(f, copy):
        pl.when(exists[f])(copy.start)
        waits.append((f, copy))

    count = count_ref[0, 0]
    lines = lax.broadcasted_iota(jnp.int32, (width, width), 0)
    orders = [(lines == maps_ref[d : d + 1, :]).astype(jnp.float32) for d in range(3)]
    own_modes[0:modes, :] = modes_ref[...]
    padded_load[0:modes, 0:cases] = coarse_ref[...]
    raw_modes = jnp.where(
        lax.broadcasted_iota(jnp.int32, own_modes.shape, 0) < count, own_modes[...], 0.0
    )
    pieces = []
    for d in range(3):
        pieces.append(masked(mul(face(raw_modes, 2 * d), orders[d], NT), 2 * d))
        pieces.append(masked(face(raw_modes, 2 * d + 1), 2 * d + 1))
    mode_rows = jnp.concatenate(pieces, axis=1)
    own_modes[...] = mode_rows
    minus_modes[...] = -mode_rows
    all_modes[0:padded, :] = mode_rows
    inactive = lax.broadcasted_iota(jnp.int32, (padded, padded), 0) >= count
    normal = mul(mode_rows, mode_rows, NT) + jnp.where(inactive, identity(padded), 0.0)
    coarse_inverse = eliminate(jnp.concatenate([normal, identity(padded)], axis=1), padded)
    active_load = jnp.where(
        lax.broadcasted_iota(jnp.int32, padded_load.shape, 0) < count, padded_load[...], 0.0
    )
    coefficients[0, 0:padded, :] = mul(coarse_inverse, active_load)

    pl.semaphore_wait(barrier, plane - 1 + nz - 1)

    def slot_of(phase, f):
        return coefficients.at[phase, pl.ds((1 + f) * padded, padded), :]

    def columns(ref, f):
        return ref.at[:, pl.ds(f * width, width)]

    def send_coefficients(phase):
        for f in range(6):
            start_to(
                f,
                remote(
                    coefficients.at[phase, pl.ds(0, padded), :],
                    slot_of(phase, f ^ 1),
                    coefficient_send.at[phase, f],
                    coefficient_recv.at[phase, f ^ 1],
                    neighbour[f],
                ),
            )

    def wait_coefficients(phase):
        for f in range(6):
            copy = remote(
                coefficients.at[phase, pl.ds(0, padded), :],
                slot_of(phase, f),
                coefficient_send.at[phase, f],
                coefficient_recv.at[phase, f],
                neighbour[f],
            )
            pl.when(exists[f])(copy.wait_recv)

    def coarse_field(phase):
        return mul(coefficients[phase][:, 0:cases], all_modes[...], TN)

    def send_faces(phase):
        for f in range(6):
            start_to(
                f,
                remote(
                    face_out.at[phase, f],
                    face_in.at[phase, f ^ 1],
                    face_send.at[phase, f],
                    face_recv.at[phase, f ^ 1],
                    neighbour[f],
                ),
            )

    def wait_faces(phase):
        for f in range(6):
            copy = remote(
                face_out.at[phase, f],
                face_in.at[phase, f],
                face_send.at[phase, f],
                face_recv.at[phase, f],
                neighbour[f],
            )
            pl.when(exists[f])(copy.wait_recv)

    def assembled(phase):
        return jnp.concatenate(
            [masked(face_out[phase, f] - face_in[phase, f], f) for f in range(6)], axis=1
        )

    def apply_local(values):
        head = values.astype(jnp.bfloat16)
        tail = (values - head.astype(jnp.float32)).astype(jnp.bfloat16)
        both = jnp.dot(
            jnp.concatenate([head, tail], axis=0),
            ordered[...],
            preferred_element_type=jnp.float32,
        )
        return both[0:cases] + both[cases:]

    def keep_faces(phase, values):
        for f in range(6):
            face_out[phase, f] = face(values, f)

    def owned(values):
        return jnp.concatenate([face(values, 1), face(values, 3), face(values, 5)], axis=1)

    for f in range(6):
        start_to(
            f,
            remote(
                columns(minus_modes, f),
                all_modes.at[pl.ds((1 + (f ^ 1)) * padded, padded), pl.ds((f ^ 1) * width, width)],
                mode_send.at[f],
                mode_recv.at[f ^ 1],
                neighbour[f],
            ),
        )
    send_coefficients(0)
    for d in range(3):
        start_to(
            2 * d + 1,
            remote(
                columns(load_ref, d),
                load_in.at[d],
                load_send.at[d],
                load_recv.at[d],
                neighbour[2 * d + 1],
            ),
        )

    fetch.wait()
    narrow = [order.astype(jnp.bfloat16) for order in orders]
    for d in range(3):
        low = 2 * d * width
        raw[pl.ds(low, width), :] = jnp.dot(
            narrow[d], raw[pl.ds(low, width), :], preferred_element_type=jnp.float32
        ).astype(jnp.bfloat16)
    for d in range(3):
        low = 2 * d * width
        ordered[:, low : low + width] = lax.dot_general(
            raw[:, low : low + width], narrow[d], NT, preferred_element_type=jnp.float32
        ).astype(jnp.bfloat16)
        ordered[:, low + width : low + 2 * width] = raw[:, low + width : low + 2 * width]
    inverse_modes = mul(coarse_inverse, mode_rows)

    for f in range(6):
        copy = remote(
            columns(minus_modes, f),
            all_modes.at[pl.ds((1 + f) * padded, padded), pl.ds(f * width, width)],
            mode_send.at[f],
            mode_recv.at[f],
            neighbour[f],
        )
        pl.when(exists[f])(copy.wait_recv)
    wait_coefficients(0)
    initial = coarse_field(0)
    product = apply_local(initial)
    keep_faces(0, product)
    send_faces(0)
    for d in range(3):
        copy = remote(
            columns(load_ref, d),
            load_in.at[d],
            load_send.at[d],
            load_recv.at[d],
            neighbour[2 * d],
        )
        pl.when(exists[2 * d])(copy.wait_recv)
    right = []
    for d in range(3):
        right.append(masked(-load_in[d], 2 * d))
        right.append(masked(load_ref[:, d * width : (d + 1) * width], 2 * d + 1))
    right = jnp.concatenate(right, axis=1)
    wait_faces(0)
    residual = right - assembled(0)

    def precondition(phase, values):
        coefficients[phase, 0:padded, 0:cases] = mul(inverse_modes, values, NT)
        send_coefficients(phase)

    def preconditioned(phase, values):
        wait_coefficients(phase)
        return values - 0.25 * coarse_field(phase)

    def sum_start(which, tile):
        plane_sums[which, slot] = tile
        copies = []
        for offset in range(1, plane):
            copy = remote(
                plane_sums.at[which, slot],
                plane_sums.at[which, slot],
                plane_send.at[which, offset],
                plane_recv.at[which, offset],
                plane_peer(offset),
            )
            copy.start()
            copies.append(copy)
        return copies

    def sum_middle(which, copies):
        for offset in range(1, plane):
            copy = remote(
                plane_sums.at[which, slot],
                plane_sums.at[which, lax.rem(slot + plane - offset, plane)],
                plane_send.at[which, offset],
                plane_recv.at[which, offset],
                plane_peer(offset),
            )
            copy.wait_recv()
        total = plane_sums[which, 0]
        for other in range(1, plane):
            total = total + plane_sums[which, other]
        line_sums[which, iz] = total
        for offset in range(1, nz):
            copy = remote(
                line_sums.at[which, iz],
                line_sums.at[which, iz],
                line_send.at[which, offset],
                line_recv.at[which, offset],
                line_peer(offset),
            )
            copy.start()
            copies.append(copy)

    def sum_end(which):
        for offset in range(1, nz):
            copy = remote(
                line_sums.at[which, iz],
                line_sums.at[which, lax.rem(iz + nz - offset, nz)],
                line_send.at[which, offset],
                line_recv.at[which, offset],
                line_peer(offset),
            )
            copy.wait_recv()
        total = line_sums[which, 0]
        for other in range(1, nz):
            total = total + line_sums[which, other]
        half = total.shape[0] // 2
        return unpacked(total[0:half], cases), unpacked(total[half:], cases)

    precondition(1, residual)
    start = preconditioned(1, residual)
    product = apply_local(start)
    keep_faces(1, product)
    send_faces(1)
    early = sum_start(
        0,
        jnp.concatenate(
            [
                packed(mul(owned(start), owned(residual), NT), width),
                packed(mul(start, product, NT), width),
            ],
            axis=0,
        ),
    )
    wait_faces(1)
    image = assembled(1)
    precondition(2, image)
    sum_middle(0, early)
    second = preconditioned(2, image)
    product = apply_local(second)
    keep_faces(2, product)
    late = sum_start(
        1,
        jnp.concatenate(
            [
                packed(mul(owned(second), owned(image), NT), width),
                packed(mul(second, product, NT), width),
            ],
            axis=0,
        ),
    )
    send_faces(2)
    gram, energy = sum_end(0)
    inverse = eliminate(jnp.concatenate([energy, identity(cases)], axis=1), cases)
    alpha = mul(inverse, gram)
    sum_middle(1, late)
    wait_faces(2)
    second_image = assembled(2)
    cross, last = sum_end(1)
    carried = mul(inverse, cross)
    schur = last - mul(cross, carried)
    right_side = mul(cross, alpha) - energy
    tail = eliminate(jnp.concatenate([schur, right_side], axis=1), cases)
    head = alpha + mul(carried, tail)
    both = jnp.concatenate([head, -tail], axis=0)
    multipliers_ref[...] = owned(initial) + mul(
        both, jnp.concatenate([owned(start), owned(second)], axis=0), TN
    )
    residual_ref[...] = owned(residual) - mul(
        both, jnp.concatenate([owned(image), owned(second_image)], axis=0), TN
    )

    for f, copy in waits:
        pl.when(exists[f])(copy.wait_send)
    for copy in early + late:
        copy.wait_send()


def local(extents, dual_operators, dual_load, rigid_modes, coarse_load, mode_counts, face_maps):
    size = dual_operators.shape[-1]
    cases = dual_load.shape[-2]
    width = dual_load.shape[-1] // 3
    modes = rigid_modes.shape[-2]
    padded = -(-modes // 8) * 8
    nx, ny, nz = extents
    plane = nx * ny
    tile = 2 * cases // max(1, width // cases)
    f32 = jnp.float32
    vmem = pl.BlockSpec(memory_space=pltpu.VMEM)
    dma = pltpu.SemaphoreType.DMA
    out = jax.ShapeDtypeStruct((cases, 3 * width), f32)
    multipliers, residual = pl.pallas_call(
        functools.partial(kernel, extents),
        out_shape=(out, out),
        in_specs=[
            pl.BlockSpec(memory_space=pl.ANY),
            vmem,
            vmem,
            vmem,
            pl.BlockSpec(memory_space=pltpu.SMEM),
            vmem,
        ],
        out_specs=(vmem, vmem),
        scratch_shapes=[
            pltpu.VMEM((size, size), dual_operators.dtype),
            pltpu.VMEM((size, size), dual_operators.dtype),
            pltpu.VMEM((padded, size), f32),
            pltpu.VMEM((padded, size), f32),
            pltpu.VMEM((7 * padded, size), f32),
            pltpu.VMEM((padded, width), f32),
            pltpu.VMEM((3, 7 * padded, width), f32),
            pltpu.VMEM((3, 6, cases, width), f32),
            pltpu.VMEM((3, 6, cases, width), f32),
            pltpu.VMEM((3, cases, width), f32),
            pltpu.VMEM((2, plane, tile, width), f32),
            pltpu.VMEM((2, nz, tile, width), f32),
            dma,
            dma((3, 6)),
            dma((3, 6)),
            dma((3, 6)),
            dma((3, 6)),
            dma((6,)),
            dma((6,)),
            dma((3,)),
            dma((3,)),
            dma((2, plane)),
            dma((2, plane)),
            dma((2, nz)),
            dma((2, nz)),
        ],
        compiler_params=pltpu.CompilerParams(collective_id=0, has_side_effects=True),
    )(
        dual_operators.reshape(size, size),
        dual_load.reshape(cases, 3 * width),
        rigid_modes.reshape(modes, size),
        coarse_load.reshape(modes, cases),
        mode_counts.reshape(1, 1),
        face_maps.reshape(3, width),
    )
    shape = (1, 1, 1, cases, 3 * width)
    return multipliers.reshape(shape), residual.reshape(shape)


def solution(mesh):
    extents = (mesh.shape["gx"], mesh.shape["gy"], mesh.shape["gz"])
    spec = P("gx", "gy", "gz", None, None)
    return jax.shard_map(
        functools.partial(local, extents),
        mesh=mesh,
        in_specs=(spec, spec, spec, spec, P("gx", "gy", "gz"), spec),
        out_specs=(spec, spec),
        check_vma=False,
    )
```

```python
import functools

import jax
import jax.numpy as jnp
from jax import lax
from jax.experimental import pallas as pl
from jax.experimental.pallas import tpu as pltpu
from jax.sharding import PartitionSpec as P

MESH = pl.DeviceIdType.MESH
HIGH = lax.Precision.HIGHEST
NN = (((1,), (0,)), ((), ()))
NT = (((1,), (1,)), ((), ()))
TN = (((0,), (0,)), ((), ()))


def mul(a, b, dims=NN):
    return lax.dot_general(a, b, dims, precision=HIGH, preferred_element_type=jnp.float32)


def eliminate(system, size):
    rows = lax.broadcasted_iota(jnp.int32, system.shape, 0)
    for k in range(size):
        row = system[k : k + 1, :]
        column = system[:, k : k + 1]
        scaled = row / row[:, k : k + 1]
        system = jnp.where(rows == k, scaled, system - column * scaled)
    return system[:, size:]


def identity(size):
    return (
        lax.broadcasted_iota(jnp.int32, (size, size), 0)
        == lax.broadcasted_iota(jnp.int32, (size, size), 1)
    ).astype(jnp.float32)


def packed(gram, width):
    groups = max(1, width // gram.shape[1])
    depth = gram.shape[0] // groups
    return jnp.concatenate([gram[g * depth : (g + 1) * depth] for g in range(groups)], axis=1)


def unpacked(tile, size):
    groups = max(1, tile.shape[1] // size)
    return jnp.concatenate([tile[:, g * size : (g + 1) * size] for g in range(groups)], axis=0)


def kernel(
    extents,
    operator_hbm,
    load_hbm,
    modes_hbm,
    coarse_hbm,
    count_ref,
    maps_hbm,
    multipliers_ref,
    residual_ref,
    raw,
    load_ref,
    modes_ref,
    coarse_ref,
    maps_ref,
    ordered,
    own_modes,
    minus_modes,
    all_modes,
    padded_load,
    coefficients,
    face_out,
    face_in,
    load_in,
    plane_sums,
    line_sums,
    raw_sem,
    coefficient_send,
    coefficient_recv,
    face_send,
    face_recv,
    mode_send,
    mode_recv,
    load_send,
    load_recv,
    plane_send,
    plane_recv,
    line_send,
    line_recv,
):
    nx, ny, nz = extents
    cases = load_hbm.shape[0]
    width = load_hbm.shape[1] // 3
    modes = modes_hbm.shape[0]
    padded = own_modes.shape[0]
    here = (lax.axis_index("gx"), lax.axis_index("gy"), lax.axis_index("gz"))
    ix, iy, iz = here
    plane = nx * ny
    slot = ix * ny + iy

    fetches = [
        pltpu.make_async_copy(source, target, raw_sem.at[i])
        for i, (source, target) in enumerate(
            (
                (maps_hbm, maps_ref),
                (modes_hbm, modes_ref),
                (coarse_hbm, coarse_ref),
                (load_hbm, load_ref),
                (operator_hbm, raw),
            )
        )
    ]
    for fetch in fetches:
        fetch.start()

    for phase in range(3):
        coefficients[phase] = jnp.zeros(coefficients.shape[1:], jnp.float32)
    all_modes[...] = jnp.zeros(all_modes.shape, jnp.float32)
    own_modes[...] = jnp.zeros(own_modes.shape, jnp.float32)
    padded_load[...] = jnp.zeros(padded_load.shape, jnp.float32)

    def plane_peer(offset):
        other = lax.rem(slot + offset, plane)
        return (lax.div(other, ny), lax.rem(other, ny), iz)

    def line_peer(offset):
        return (ix, iy, lax.rem(iz + offset, nz))

    barrier = pltpu.get_barrier_semaphore()
    for offset in range(1, plane):
        pl.semaphore_signal(barrier, inc=1, device_id=plane_peer(offset), device_id_type=MESH)
    for offset in range(1, nz):
        pl.semaphore_signal(barrier, inc=1, device_id=line_peer(offset), device_id_type=MESH)

    exists = []
    neighbour = []
    for d in range(3):
        exists.append(here[d] > 0)
        exists.append(here[d] < extents[d] - 1)
        for step in (-1, 1):
            neighbour.append(tuple(here[a] + (step if a == d else 0) for a in range(3)))
    flags = [jnp.where(e, 1, 0).astype(jnp.int32) for e in exists]

    def face(values, f):
        return values[:, f * width : (f + 1) * width]

    def masked(values, f):
        return jnp.where(jnp.full(values.shape, flags[f], jnp.int32) == 1, values, 0.0)

    waits = []

    def remote(source, target, send, recv, where):
        return pltpu.make_async_remote_copy(
            src_ref=source,
            dst_ref=target,
            send_sem=send,
            recv_sem=recv,
            device_id=where,
            device_id_type=MESH,
        )

    def start_to(f, copy):
        pl.when(exists[f])(copy.start)
        waits.append((f, copy))

    for fetch in fetches[:4]:
        fetch.wait()
    count = count_ref[0, 0]
    lines = lax.broadcasted_iota(jnp.int32, (width, width), 0)
    orders = [(lines == maps_ref[d]).astype(jnp.float32) for d in range(3)]
    for m in range(modes):
        own_modes[m : m + 1, :] = modes_ref[m]
        padded_load[m : m + 1, 0:cases] = coarse_ref[m]
    raw_modes = jnp.where(
        lax.broadcasted_iota(jnp.int32, own_modes.shape, 0) < count, own_modes[...], 0.0
    )
    pieces = []
    for d in range(3):
        pieces.append(masked(mul(face(raw_modes, 2 * d), orders[d], NT), 2 * d))
        pieces.append(masked(face(raw_modes, 2 * d + 1), 2 * d + 1))
    mode_rows = jnp.concatenate(pieces, axis=1)
    own_modes[...] = mode_rows
    minus_modes[...] = -mode_rows
    all_modes[0:padded, :] = mode_rows
    inactive = lax.broadcasted_iota(jnp.int32, (padded, padded), 0) >= count
    normal = mul(mode_rows, mode_rows, NT) + jnp.where(inactive, identity(padded), 0.0)
    coarse_inverse = eliminate(jnp.concatenate([normal, identity(padded)], axis=1), padded)
    active_load = jnp.where(
        lax.broadcasted_iota(jnp.int32, padded_load.shape, 0) < count, padded_load[...], 0.0
    )
    coefficients[0, 0:padded, :] = mul(coarse_inverse, active_load)

    pl.semaphore_wait(barrier, plane - 1 + nz - 1)

    def slot_of(phase, f):
        return coefficients.at[phase, pl.ds((1 + f) * padded, padded), :]

    def columns(ref, f):
        return ref.at[:, pl.ds(f * width, width)]

    def send_coefficients(phase):
        for f in range(6):
            start_to(
                f,
                remote(
                    coefficients.at[phase, pl.ds(0, padded), :],
                    slot_of(phase, f ^ 1),
                    coefficient_send.at[phase, f],
                    coefficient_recv.at[phase, f ^ 1],
                    neighbour[f],
                ),
            )

    def wait_coefficients(phase):
        for f in range(6):
            copy = remote(
                coefficients.at[phase, pl.ds(0, padded), :],
                slot_of(phase, f),
                coefficient_send.at[phase, f],
                coefficient_recv.at[phase, f],
                neighbour[f],
            )
            pl.when(exists[f])(copy.wait_recv)

    def coarse_field(phase):
        return mul(coefficients[phase][:, 0:cases], all_modes[...], TN)

    def send_faces(phase):
        for f in range(6):
            start_to(
                f,
                remote(
                    face_out.at[phase, f],
                    face_in.at[phase, f ^ 1],
                    face_send.at[phase, f],
                    face_recv.at[phase, f ^ 1],
                    neighbour[f],
                ),
            )

    def wait_faces(phase):
        for f in range(6):
            copy = remote(
                face_out.at[phase, f],
                face_in.at[phase, f],
                face_send.at[phase, f],
                face_recv.at[phase, f],
                neighbour[f],
            )
            pl.when(exists[f])(copy.wait_recv)

    def assembled(phase):
        return jnp.concatenate(
            [masked(face_out[phase, f] - face_in[phase, f], f) for f in range(6)], axis=1
        )

    def apply_local(values):
        head = values.astype(jnp.bfloat16)
        tail = (values - head.astype(jnp.float32)).astype(jnp.bfloat16)
        both = jnp.dot(
            jnp.concatenate([head, tail], axis=0),
            ordered[...],
            preferred_element_type=jnp.float32,
        )
        return both[0:cases] + both[cases:]

    def keep_faces(phase, values):
        for f in range(6):
            face_out[phase, f] = face(values, f)

    def owned(values):
        return jnp.concatenate([face(values, 1), face(values, 3), face(values, 5)], axis=1)

    for f in range(6):
        start_to(
            f,
            remote(
                columns(minus_modes, f),
                all_modes.at[pl.ds((1 + (f ^ 1)) * padded, padded), pl.ds((f ^ 1) * width, width)],
                mode_send.at[f],
                mode_recv.at[f ^ 1],
                neighbour[f],
            ),
        )
    send_coefficients(0)
    for d in range(3):
        start_to(
            2 * d + 1,
            remote(
                columns(load_ref, d),
                load_in.at[d],
                load_send.at[d],
                load_recv.at[d],
                neighbour[2 * d + 1],
            ),
        )

    fetches[4].wait()
    narrow = [order.astype(jnp.bfloat16) for order in orders]
    for d in range(3):
        low = 2 * d * width
        raw[pl.ds(low, width), :] = jnp.dot(
            narrow[d], raw[pl.ds(low, width), :], preferred_element_type=jnp.float32
        ).astype(jnp.bfloat16)
    for d in range(3):
        low = 2 * d * width
        ordered[:, low : low + width] = lax.dot_general(
            raw[:, low : low + width], narrow[d], NT, preferred_element_type=jnp.float32
        ).astype(jnp.bfloat16)
        ordered[:, low + width : low + 2 * width] = raw[:, low + width : low + 2 * width]
    inverse_modes = mul(coarse_inverse, mode_rows)

    for f in range(6):
        copy = remote(
            columns(minus_modes, f),
            all_modes.at[pl.ds((1 + f) * padded, padded), pl.ds(f * width, width)],
            mode_send.at[f],
            mode_recv.at[f],
            neighbour[f],
        )
        pl.when(exists[f])(copy.wait_recv)
    wait_coefficients(0)
    initial = coarse_field(0)
    product = apply_local(initial)
    keep_faces(0, product)
    send_faces(0)
    for d in range(3):
        copy = remote(
            columns(load_ref, d),
            load_in.at[d],
            load_send.at[d],
            load_recv.at[d],
            neighbour[2 * d],
        )
        pl.when(exists[2 * d])(copy.wait_recv)
    right = []
    for d in range(3):
        right.append(masked(-load_in[d], 2 * d))
        right.append(masked(load_ref[:, d * width : (d + 1) * width], 2 * d + 1))
    right = jnp.concatenate(right, axis=1)
    wait_faces(0)
    residual = right - assembled(0)

    def precondition(phase, values):
        coefficients[phase, 0:padded, 0:cases] = mul(inverse_modes, values, NT)
        send_coefficients(phase)

    def preconditioned(phase, values):
        wait_coefficients(phase)
        return values - 0.25 * coarse_field(phase)

    def sum_start(which, tile):
        plane_sums[which, slot] = tile
        copies = []
        for offset in range(1, plane):
            copy = remote(
                plane_sums.at[which, slot],
                plane_sums.at[which, slot],
                plane_send.at[which, offset],
                plane_recv.at[which, offset],
                plane_peer(offset),
            )
            copy.start()
            copies.append(copy)
        return copies

    def sum_middle(which, copies):
        for offset in range(1, plane):
            copy = remote(
                plane_sums.at[which, slot],
                plane_sums.at[which, lax.rem(slot + plane - offset, plane)],
                plane_send.at[which, offset],
                plane_recv.at[which, offset],
                plane_peer(offset),
            )
            copy.wait_recv()
        total = plane_sums[which, 0]
        for other in range(1, plane):
            total = total + plane_sums[which, other]
        line_sums[which, iz] = total
        for offset in range(1, nz):
            copy = remote(
                line_sums.at[which, iz],
                line_sums.at[which, iz],
                line_send.at[which, offset],
                line_recv.at[which, offset],
                line_peer(offset),
            )
            copy.start()
            copies.append(copy)

    def sum_end(which):
        for offset in range(1, nz):
            copy = remote(
                line_sums.at[which, iz],
                line_sums.at[which, lax.rem(iz + nz - offset, nz)],
                line_send.at[which, offset],
                line_recv.at[which, offset],
                line_peer(offset),
            )
            copy.wait_recv()
        total = line_sums[which, 0]
        for other in range(1, nz):
            total = total + line_sums[which, other]
        half = total.shape[0] // 2
        return unpacked(total[0:half], cases), unpacked(total[half:], cases)

    precondition(1, residual)
    start = preconditioned(1, residual)
    product = apply_local(start)
    keep_faces(1, product)
    send_faces(1)
    early = sum_start(
        0,
        jnp.concatenate(
            [
                packed(mul(owned(start), owned(residual), NT), width),
                packed(mul(start, product, NT), width),
            ],
            axis=0,
        ),
    )
    wait_faces(1)
    image = assembled(1)
    precondition(2, image)
    sum_middle(0, early)
    second = preconditioned(2, image)
    product = apply_local(second)
    keep_faces(2, product)
    late = sum_start(
        1,
        jnp.concatenate(
            [
                packed(mul(owned(second), owned(image), NT), width),
                packed(mul(second, product, NT), width),
            ],
            axis=0,
        ),
    )
    send_faces(2)
    gram, energy = sum_end(0)
    inverse = eliminate(jnp.concatenate([energy, identity(cases)], axis=1), cases)
    alpha = mul(inverse, gram)
    sum_middle(1, late)
    wait_faces(2)
    second_image = assembled(2)
    cross, last = sum_end(1)
    carried = mul(inverse, cross)
    schur = last - mul(cross, carried)
    right_side = mul(cross, alpha) - energy
    tail = eliminate(jnp.concatenate([schur, right_side], axis=1), cases)
    head = alpha + mul(carried, tail)
    both = jnp.concatenate([head, -tail], axis=0)
    multipliers_ref[...] = owned(initial) + mul(
        both, jnp.concatenate([owned(start), owned(second)], axis=0), TN
    )
    residual_ref[...] = owned(residual) - mul(
        both, jnp.concatenate([owned(image), owned(second_image)], axis=0), TN
    )

    for f, copy in waits:
        pl.when(exists[f])(copy.wait_send)
    for copy in early + late:
        copy.wait_send()


def held(array):
    return pltpu.with_memory_space_constraint(array, pltpu.HBM)


def rows_apart(array):
    return jnp.swapaxes(array, 2, 3).reshape(array.shape[3], 1, array.shape[4])


def local(extents, dual_operators, dual_load, rigid_modes, coarse_load, mode_counts, face_maps):
    size = dual_operators.shape[-1]
    cases = dual_load.shape[-2]
    width = dual_load.shape[-1] // 3
    modes = rigid_modes.shape[-2]
    padded = -(-modes // 8) * 8
    nx, ny, nz = extents
    plane = nx * ny
    tile = 2 * cases // max(1, width // cases)
    f32 = jnp.float32
    vmem = pl.BlockSpec(memory_space=pltpu.VMEM)
    hbm = pl.BlockSpec(memory_space=pltpu.HBM)
    dma = pltpu.SemaphoreType.DMA
    out = jax.ShapeDtypeStruct((cases, 3 * width), f32)
    multipliers, residual = pl.pallas_call(
        functools.partial(kernel, extents),
        out_shape=(out, out),
        in_specs=[
            hbm,
            hbm,
            hbm,
            hbm,
            pl.BlockSpec(memory_space=pltpu.SMEM),
            hbm,
        ],
        out_specs=(vmem, vmem),
        scratch_shapes=[
            pltpu.VMEM((size, size), dual_operators.dtype),
            pltpu.VMEM((cases, 3 * width), f32),
            pltpu.VMEM((modes, 1, size), f32),
            pltpu.VMEM((modes, 1, cases), f32),
            pltpu.VMEM((3, 1, width), jnp.int32),
            pltpu.VMEM((size, size), dual_operators.dtype),
            pltpu.VMEM((padded, size), f32),
            pltpu.VMEM((padded, size), f32),
            pltpu.VMEM((7 * padded, size), f32),
            pltpu.VMEM((padded, width), f32),
            pltpu.VMEM((3, 7 * padded, width), f32),
            pltpu.VMEM((3, 6, cases, width), f32),
            pltpu.VMEM((3, 6, cases, width), f32),
            pltpu.VMEM((3, cases, width), f32),
            pltpu.VMEM((2, plane, tile, width), f32),
            pltpu.VMEM((2, nz, tile, width), f32),
            dma((5,)),
            dma((3, 6)),
            dma((3, 6)),
            dma((3, 6)),
            dma((3, 6)),
            dma((6,)),
            dma((6,)),
            dma((3,)),
            dma((3,)),
            dma((2, plane)),
            dma((2, plane)),
            dma((2, nz)),
            dma((2, nz)),
        ],
        compiler_params=pltpu.CompilerParams(collective_id=0, has_side_effects=True, vmem_limit_bytes=16 * 1024 * 1024
        ),
    )(
        held(dual_operators.reshape(size, size)),
        held(dual_load.reshape(cases, 3 * width)),
        held(rows_apart(rigid_modes)),
        held(rows_apart(coarse_load)),
        mode_counts.reshape(1, 1),
        held(rows_apart(face_maps)),
    )
    shape = (1, 1, 1, cases, 3 * width)
    return multipliers.reshape(shape), residual.reshape(shape)


def solution(mesh):
    extents = (mesh.shape["gx"], mesh.shape["gy"], mesh.shape["gz"])
    spec = P("gx", "gy", "gz", None, None)
    return jax.shard_map(
        functools.partial(local, extents),
        mesh=mesh,
        in_specs=(spec, spec, spec, spec, P("gx", "gy", "gz"), spec),
        out_specs=(spec, spec),
        check_vma=False,
    )
```

```python
import functools

import jax
import jax.numpy as jnp
from jax import lax
from jax.experimental import pallas as pl
from jax.experimental.pallas import tpu as pltpu
from jax.sharding import PartitionSpec as P

MESH = pl.DeviceIdType.MESH
HIGH = lax.Precision.HIGHEST
NN = (((1,), (0,)), ((), ()))
NT = (((1,), (1,)), ((), ()))
TN = (((0,), (0,)), ((), ()))


def mul(a, b, dims=NN):
    return lax.dot_general(a, b, dims, precision=HIGH, preferred_element_type=jnp.float32)


def eliminate(system, size):
    rows = lax.broadcasted_iota(jnp.int32, system.shape, 0)
    for k in range(size):
        row = system[k : k + 1, :]
        column = system[:, k : k + 1]
        scaled = row / row[:, k : k + 1]
        system = jnp.where(rows == k, scaled, system - column * scaled)
    return system[:, size:]


def identity(size):
    return (
        lax.broadcasted_iota(jnp.int32, (size, size), 0)
        == lax.broadcasted_iota(jnp.int32, (size, size), 1)
    ).astype(jnp.float32)


def packed(gram, width):
    groups = max(1, width // gram.shape[1])
    depth = gram.shape[0] // groups
    return jnp.concatenate([gram[g * depth : (g + 1) * depth] for g in range(groups)], axis=1)


def unpacked(tile, size):
    groups = max(1, tile.shape[1] // size)
    return jnp.concatenate([tile[:, g * size : (g + 1) * size] for g in range(groups)], axis=0)


def kernel(
    extents,
    operator_hbm,
    load_hbm,
    modes_hbm,
    coarse_hbm,
    count_ref,
    maps_hbm,
    multipliers_ref,
    residual_ref,
    raw,
    load_ref,
    modes_ref,
    coarse_ref,
    maps_ref,
    ordered,
    own_modes,
    all_modes,
    padded_load,
    probes,
    first_out,
    first_in,
    pair_out,
    pair_in,
    face_out,
    face_in,
    last_out,
    last_in,
    load_in,
    plane_sums,
    line_sums,
    raw_sem,
    first_send,
    first_recv,
    face_send,
    face_recv,
    pair_send,
    pair_recv,
    last_send,
    last_recv,
    load_send,
    load_recv,
    plane_send,
    plane_recv,
    line_send,
    line_recv,
):
    nx, ny, nz = extents
    cases = load_hbm.shape[0]
    width = load_hbm.shape[1] // 3
    modes = modes_hbm.shape[0]
    padded = own_modes.shape[0]
    here = (lax.axis_index("gx"), lax.axis_index("gy"), lax.axis_index("gz"))
    ix, iy, iz = here
    plane = nx * ny
    slot = ix * ny + iy

    fetches = [
        pltpu.make_async_copy(source, target, raw_sem.at[i])
        for i, (source, target) in enumerate(
            (
                (maps_hbm, maps_ref),
                (modes_hbm, modes_ref),
                (coarse_hbm, coarse_ref),
                (load_hbm, load_ref),
                (operator_hbm, raw),
            )
        )
    ]
    for fetch in fetches:
        fetch.start()

    all_modes[...] = jnp.zeros(all_modes.shape, jnp.float32)
    probes[...] = jnp.zeros(probes.shape, jnp.float32)
    first_in[...] = jnp.zeros(first_in.shape, jnp.float32)
    pair_in[...] = jnp.zeros(pair_in.shape, jnp.float32)
    pair_out[...] = jnp.zeros(pair_out.shape, jnp.float32)
    face_out[:, :, cases:, :] = jnp.zeros((2, 6, padded, width), jnp.float32)
    face_in[:, :, cases:, :] = jnp.zeros((2, 6, padded, width), jnp.float32)
    own_modes[...] = jnp.zeros(own_modes.shape, jnp.float32)
    padded_load[...] = jnp.zeros(padded_load.shape, jnp.float32)

    def plane_peer(offset):
        other = lax.rem(slot + offset, plane)
        return (lax.div(other, ny), lax.rem(other, ny), iz)

    def line_peer(offset):
        return (ix, iy, lax.rem(iz + offset, nz))

    exists = []
    neighbour = []
    for d in range(3):
        exists.append(here[d] > 0)
        exists.append(here[d] < extents[d] - 1)
        for step in (-1, 1):
            neighbour.append(tuple(here[a] + (step if a == d else 0) for a in range(3)))
    flags = [jnp.where(e, 1, 0).astype(jnp.int32) for e in exists]

    def moved(position, f):
        return tuple(position[a] + ((2 * (f % 2) - 1) if a == f // 2 else 0) for a in range(3))

    def both_exist(f, g):
        if f != g:
            return jnp.logical_and(exists[f], exists[g])
        if f % 2:
            return here[f // 2] < extents[f // 2] - 2
        return here[f // 2] > 1

    pairs = [
        (f, g)
        for f in range(6)
        for g in range(6)
        if (f == g or f // 2 < g // 2) and extents[f // 2] > 1 + (f == g) and extents[g // 2] > 1
    ]

    barrier = pltpu.get_barrier_semaphore()
    diagonal = 0
    for f in range(4):
        for g in range(4, 6):
            peer = moved(moved(here, f), g)

            @pl.when(both_exist(f, g))
            def _(peer=peer):
                pl.semaphore_signal(barrier, inc=1, device_id=peer, device_id_type=MESH)

            diagonal = diagonal + flags[f] * flags[g]
    for offset in range(1, plane):
        pl.semaphore_signal(barrier, inc=1, device_id=plane_peer(offset), device_id_type=MESH)
    for offset in range(1, nz):
        pl.semaphore_signal(barrier, inc=1, device_id=line_peer(offset), device_id_type=MESH)


    def face(values, f):
        return values[:, f * width : (f + 1) * width]

    def masked(values, f):
        return jnp.where(jnp.full(values.shape, flags[f], jnp.int32) == 1, values, 0.0)

    sends = [[] for _ in range(6)]
    pair_sends = [[] for _ in pairs]

    def remote(source, target, send, recv, where):
        return pltpu.make_async_remote_copy(
            src_ref=source,
            dst_ref=target,
            send_sem=send,
            recv_sem=recv,
            device_id=where,
            device_id_type=MESH,
        )

    def start_to(f, copies):
        @pl.when(exists[f])
        def _():
            for copy in copies:
                copy.start()

        sends[f].extend(copies)

    for fetch in fetches[:4]:
        fetch.wait()
    count = count_ref[0, 0]
    lines = lax.broadcasted_iota(jnp.int32, (width, width), 0)
    orders = [(lines == maps_ref[d]).astype(jnp.float32) for d in range(3)]
    for m in range(modes):
        own_modes[m : m + 1, :] = modes_ref[m]
        padded_load[m : m + 1, 0:cases] = coarse_ref[m]
    raw_modes = jnp.where(
        lax.broadcasted_iota(jnp.int32, own_modes.shape, 0) < count, own_modes[...], 0.0
    )
    pieces = []
    for d in range(3):
        pieces.append(masked(mul(face(raw_modes, 2 * d), orders[d], NT), 2 * d))
        pieces.append(masked(face(raw_modes, 2 * d + 1), 2 * d + 1))
    mode_rows = jnp.concatenate(pieces, axis=1)
    own_modes[...] = mode_rows
    all_modes[0:padded, :] = mode_rows
    inactive = lax.broadcasted_iota(jnp.int32, (padded, padded), 0) >= count
    normal = mul(mode_rows, mode_rows, NT) + jnp.where(inactive, identity(padded), 0.0)
    coarse_inverse = eliminate(jnp.concatenate([normal, identity(padded)], axis=1), padded)
    active_load = jnp.where(
        lax.broadcasted_iota(jnp.int32, padded_load.shape, 0) < count, padded_load[...], 0.0
    )
    first_part = mul(coarse_inverse, active_load)
    inverse_modes = mul(coarse_inverse, mode_rows)
    probes[6 * padded :, :] = inverse_modes
    for f in range(6):
        first_out[f, 0:padded, :] = -face(mode_rows, f)
        first_out[f, padded : 2 * padded, :] = face(inverse_modes, f)
        first_out[f, 2 * padded :, :] = first_part

    pl.semaphore_wait(barrier, plane - 1 + nz - 1 + diagonal)

    for f in range(6):
        copies = [
            remote(first_out.at[f], first_in.at[f ^ 1], first_send.at[f], first_recv.at[f ^ 1], neighbour[f])
        ]
        if f % 2:
            d = f // 2
            copies.append(
                remote(
                    load_ref.at[:, pl.ds(d * width, width)],
                    load_in.at[d],
                    load_send.at[d],
                    load_recv.at[d],
                    neighbour[f],
                )
            )
        start_to(f, copies)

    def send_round(phase, values, own=None):
        found = mul(probes[...], values, NT)
        share = found[6 * padded :] if own is None else own - found[6 * padded :]
        for f in range(6):
            face_out[phase, f, 0:cases, :] = face(values, f)
            face_out[phase, f, cases:, 0:cases] = share
        for f in range(6):
            start_to(
                f,
                [
                    remote(
                        face_out.at[phase, f],
                        face_in.at[phase, f ^ 1],
                        face_send.at[phase, f],
                        face_recv.at[phase, f ^ 1],
                        neighbour[f],
                    )
                ],
            )
        for index, (f, g) in enumerate(pairs):
            pair_out[phase, index, 0:padded, 0:cases] = found[f * padded : (f + 1) * padded]
            if f != g:
                pair_out[phase, index, padded:, 0:cases] = found[g * padded : (g + 1) * padded]
        for index, (f, g) in enumerate(pairs):
            other = pairs.index((f ^ 1, g ^ 1))
            copy = remote(
                pair_out.at[phase, index],
                pair_in.at[phase, other],
                pair_send.at[phase, index],
                pair_recv.at[phase, other],
                moved(moved(here, f), g),
            )
            pl.when(both_exist(f, g))(copy.start)
            pair_sends[index].append(copy)
        return found

    def wait_faces(phase, source, target, send, recv):
        for f in range(6):
            copy = remote(
                source.at[phase, f], target.at[phase, f], send.at[phase, f], recv.at[phase, f], neighbour[f]
            )
            pl.when(exists[f])(copy.wait_recv)

    def wait_pairs(phase):
        for index, (f, g) in enumerate(pairs):
            copy = remote(
                pair_out.at[phase, index],
                pair_in.at[phase, index],
                pair_send.at[phase, index],
                pair_recv.at[phase, index],
                moved(moved(here, f), g),
            )
            pl.when(both_exist(f, g))(copy.wait_recv)

    def assembled(mine, theirs, phase):
        return jnp.concatenate(
            [
                masked(mine[phase, f, 0:cases, :] - theirs[phase, f, 0:cases, :], f)
                for f in range(6)
            ],
            axis=1,
        )

    def apply_local(values):
        head = values.astype(jnp.bfloat16)
        tail = (values - head.astype(jnp.float32)).astype(jnp.bfloat16)
        both = jnp.dot(
            jnp.concatenate([head, tail], axis=0),
            ordered[...],
            preferred_element_type=jnp.float32,
        )
        return both[0:cases] + both[cases:]

    def owned(values):
        return jnp.concatenate([face(values, 1), face(values, 3), face(values, 5)], axis=1)

    fetches[4].wait()
    narrow = [order.astype(jnp.bfloat16) for order in orders]
    for d in range(3):
        low = 2 * d * width
        raw[pl.ds(low, width), :] = jnp.dot(
            narrow[d], raw[pl.ds(low, width), :], preferred_element_type=jnp.float32
        ).astype(jnp.bfloat16)
    for d in range(3):
        low = 2 * d * width
        ordered[:, low : low + width] = lax.dot_general(
            raw[:, low : low + width], narrow[d], NT, preferred_element_type=jnp.float32
        ).astype(jnp.bfloat16)
        ordered[:, low + width : low + 2 * width] = raw[:, low + width : low + 2 * width]
    for f in range(6):
        d = f // 2
        first = remote(first_out.at[f], first_in.at[f], first_send.at[f], first_recv.at[f], neighbour[f])
        pl.when(exists[f])(first.wait_recv)
    coefficients = [first_part]
    for f in range(6):
        all_modes[(1 + f) * padded : (2 + f) * padded, f * width : (f + 1) * width] = first_in[
            f, 0:padded, :
        ]
        probes[f * padded : (f + 1) * padded, f * width : (f + 1) * width] = first_in[
            f, padded : 2 * padded, :
        ]
        coefficients.append(first_in[f, 2 * padded :, :])
    initial = mul(jnp.concatenate(coefficients, axis=0)[:, 0:cases], all_modes[...], TN)
    product = apply_local(initial)
    right = []
    for d in range(3):
        copy = remote(
            load_ref.at[:, pl.ds(d * width, width)],
            load_in.at[d],
            load_send.at[d],
            load_recv.at[d],
            neighbour[2 * d],
        )
        pl.when(exists[2 * d])(copy.wait_recv)
    for d in range(3):
        right.append(masked(-load_in[d], 2 * d))
        right.append(masked(load_ref[:, d * width : (d + 1) * width], 2 * d + 1))
    right = jnp.concatenate(right, axis=1)
    found = send_round(0, product, mul(inverse_modes, right, NT))
    wait_faces(0, face_out, face_in, face_send, face_recv)
    residual = right - assembled(face_out, face_in, 0)

    def preconditioned(phase, values, found, sign):
        own = mul(inverse_modes, values, NT)
        wait_pairs(phase)
        terms = [found[f * padded : (f + 1) * padded] for f in range(6)]
        for index, (a, b) in enumerate(pairs):
            terms[b] = terms[b] + pair_in[phase, index, 0:padded, 0:cases]
            if a != b:
                terms[a] = terms[a] + pair_in[phase, index, padded:, 0:cases]
        every = [own]
        for f in range(6):
            every.append(face_in[phase, f, cases:, 0:cases] - sign * terms[f])
        return values - 0.25 * mul(jnp.concatenate(every, axis=0), all_modes[...], TN)

    def sum_start(which, tile):
        plane_sums[which, slot] = tile
        copies = []
        for offset in range(1, plane):
            copy = remote(
                plane_sums.at[which, slot],
                plane_sums.at[which, slot],
                plane_send.at[which, offset],
                plane_recv.at[which, offset],
                plane_peer(offset),
            )
            copy.start()
            copies.append(copy)
        return copies

    def sum_middle(which, copies):
        for offset in range(1, plane):
            copy = remote(
                plane_sums.at[which, slot],
                plane_sums.at[which, lax.rem(slot + plane - offset, plane)],
                plane_send.at[which, offset],
                plane_recv.at[which, offset],
                plane_peer(offset),
            )
            copy.wait_recv()
        total = plane_sums[which, 0]
        for other in range(1, plane):
            total = total + plane_sums[which, other]
        line_sums[which, iz] = total
        for offset in range(1, nz):
            copy = remote(
                line_sums.at[which, iz],
                line_sums.at[which, iz],
                line_send.at[which, offset],
                line_recv.at[which, offset],
                line_peer(offset),
            )
            copy.start()
            copies.append(copy)

    def sum_end(which):
        for offset in range(1, nz):
            copy = remote(
                line_sums.at[which, iz],
                line_sums.at[which, lax.rem(iz + nz - offset, nz)],
                line_send.at[which, offset],
                line_recv.at[which, offset],
                line_peer(offset),
            )
            copy.wait_recv()
        total = line_sums[which, 0]
        for other in range(1, nz):
            total = total + line_sums[which, other]
        half = total.shape[0] // 2
        return unpacked(total[0:half], cases), unpacked(total[half:], cases)

    start = preconditioned(0, residual, found, -1.0)
    product = apply_local(start)
    found = send_round(1, product)
    early = sum_start(
        0,
        jnp.concatenate(
            [
                packed(mul(owned(start), owned(residual), NT), width),
                packed(mul(start, product, NT), width),
            ],
            axis=0,
        ),
    )
    wait_faces(1, face_out, face_in, face_send, face_recv)
    image = assembled(face_out, face_in, 1)
    second = preconditioned(1, image, found, 1.0)
    sum_middle(0, early)
    product = apply_local(second)
    late = sum_start(
        1,
        jnp.concatenate(
            [
                packed(mul(owned(second), owned(image), NT), width),
                packed(mul(second, product, NT), width),
            ],
            axis=0,
        ),
    )
    for f in range(6):
        last_out[0, f] = face(product, f)
    for f in range(6):
        start_to(
            f,
            [
                remote(
                    last_out.at[0, f],
                    last_in.at[0, f ^ 1],
                    last_send.at[0, f],
                    last_recv.at[0, f ^ 1],
                    neighbour[f],
                )
            ],
        )
    gram, energy = sum_end(0)
    inverse = eliminate(jnp.concatenate([energy, identity(cases)], axis=1), cases)
    alpha = mul(inverse, gram)
    sum_middle(1, late)
    wait_faces(0, last_out, last_in, last_send, last_recv)
    second_image = assembled(last_out, last_in, 0)
    cross, last = sum_end(1)
    carried = mul(inverse, cross)
    schur = last - mul(cross, carried)
    right_side = mul(cross, alpha) - energy
    tail = eliminate(jnp.concatenate([schur, right_side], axis=1), cases)
    head = alpha + mul(carried, tail)
    both = jnp.concatenate([head, -tail], axis=0)
    multipliers_ref[...] = owned(initial) + mul(
        both, jnp.concatenate([owned(start), owned(second)], axis=0), TN
    )
    residual_ref[...] = owned(residual) - mul(
        both, jnp.concatenate([owned(image), owned(second_image)], axis=0), TN
    )

    def finish(condition, copies):
        @pl.when(condition)
        def _():
            for copy in copies:
                copy.wait_send()

    for f in range(6):
        finish(exists[f], sends[f])
    for index, (f, g) in enumerate(pairs):
        finish(both_exist(f, g), pair_sends[index])
    for copy in early + late:
        copy.wait_send()


def held(array):
    return pltpu.with_memory_space_constraint(array, pltpu.HBM)


def rows_apart(array):
    return jnp.swapaxes(array, 2, 3).reshape(array.shape[3], 1, array.shape[4])


def local(extents, dual_operators, dual_load, rigid_modes, coarse_load, mode_counts, face_maps):
    size = dual_operators.shape[-1]
    cases = dual_load.shape[-2]
    width = dual_load.shape[-1] // 3
    modes = rigid_modes.shape[-2]
    padded = -(-modes // 8) * 8
    nx, ny, nz = extents
    plane = nx * ny
    tile = 2 * cases // max(1, width // cases)
    f32 = jnp.float32
    vmem = pl.BlockSpec(memory_space=pltpu.VMEM)
    hbm = pl.BlockSpec(memory_space=pltpu.HBM)
    dma = pltpu.SemaphoreType.DMA
    out = jax.ShapeDtypeStruct((cases, 3 * width), f32)
    multipliers, residual = pl.pallas_call(
        functools.partial(kernel, extents),
        out_shape=(out, out),
        in_specs=[
            hbm,
            hbm,
            hbm,
            hbm,
            pl.BlockSpec(memory_space=pltpu.SMEM),
            hbm,
        ],
        out_specs=(vmem, vmem),
        scratch_shapes=[
            pltpu.VMEM((size, size), dual_operators.dtype),
            pltpu.VMEM((cases, 3 * width), f32),
            pltpu.VMEM((modes, 1, size), f32),
            pltpu.VMEM((modes, 1, cases), f32),
            pltpu.VMEM((3, 1, width), jnp.int32),
            pltpu.VMEM((size, size), dual_operators.dtype),
            pltpu.VMEM((padded, size), f32),
            pltpu.VMEM((7 * padded, size), f32),
            pltpu.VMEM((padded, width), f32),
            pltpu.VMEM((7 * padded, size), f32),
            pltpu.VMEM((6, 3 * padded, width), f32),
            pltpu.VMEM((6, 3 * padded, width), f32),
            pltpu.VMEM((2, 18, 2 * padded, width), f32),
            pltpu.VMEM((2, 18, 2 * padded, width), f32),
            pltpu.VMEM((2, 6, cases + padded, width), f32),
            pltpu.VMEM((2, 6, cases + padded, width), f32),
            pltpu.VMEM((1, 6, cases, width), f32),
            pltpu.VMEM((1, 6, cases, width), f32),
            pltpu.VMEM((3, cases, width), f32),
            pltpu.VMEM((2, plane, tile, width), f32),
            pltpu.VMEM((2, nz, tile, width), f32),
            dma((5,)),
            dma((6,)),
            dma((6,)),
            dma((2, 6)),
            dma((2, 6)),
            dma((2, 18)),
            dma((2, 18)),
            dma((1, 6)),
            dma((1, 6)),
            dma((3,)),
            dma((3,)),
            dma((2, plane)),
            dma((2, plane)),
            dma((2, nz)),
            dma((2, nz)),
        ],
        compiler_params=pltpu.CompilerParams(collective_id=0, has_side_effects=True, vmem_limit_bytes=16 * 1024 * 1024
        ),
    )(
        held(dual_operators.reshape(size, size)),
        held(dual_load.reshape(cases, 3 * width)),
        held(rows_apart(rigid_modes)),
        held(rows_apart(coarse_load)),
        mode_counts.reshape(1, 1),
        held(rows_apart(face_maps)),
    )
    shape = (1, 1, 1, cases, 3 * width)
    return multipliers.reshape(shape), residual.reshape(shape)


def solution(mesh):
    extents = (mesh.shape["gx"], mesh.shape["gy"], mesh.shape["gz"])
    spec = P("gx", "gy", "gz", None, None)
    return jax.shard_map(
        functools.partial(local, extents),
        mesh=mesh,
        in_specs=(spec, spec, spec, spec, P("gx", "gy", "gz"), spec),
        out_specs=(spec, spec),
        check_vma=False,
    )
```

```python
import functools

import jax
import jax.numpy as jnp
from jax import lax
from jax.experimental import pallas as pl
from jax.experimental.pallas import tpu as pltpu
from jax.sharding import PartitionSpec as P

MESH = pl.DeviceIdType.MESH
HIGH = lax.Precision.HIGHEST
NN = (((1,), (0,)), ((), ()))
NT = (((1,), (1,)), ((), ()))
TN = (((0,), (0,)), ((), ()))


def mul(a, b, dims=NN):
    return lax.dot_general(a, b, dims, precision=HIGH, preferred_element_type=jnp.float32)


def split(a):
    head = a.astype(jnp.bfloat16)
    return head, (a - head.astype(jnp.float32)).astype(jnp.bfloat16)


def fast(a, b, dims=NN):
    if dims == TN:
        a, dims = a.T, NN
    (ah, al), (bh, bl) = split(a), split(b)
    dot = functools.partial(
        lax.dot_general, dimension_numbers=dims, preferred_element_type=jnp.float32
    )
    return dot(ah, bh) + (dot(ah, bl) + dot(al, bh))


def eliminate(system, size, block=4):
    rows = lax.broadcasted_iota(jnp.int32, system.shape, 0)
    span = range(block)
    for k in range(0, size, block):
        columns = [system[:, k + j : k + j + 1] for j in span]
        lines = [system[k + i : k + i + 1, :] for i in span]
        pivots = [
            [jnp.broadcast_to(lines[i][:, k + j : k + j + 1], lines[i].shape) for j in span]
            for i in span
        ]
        for j in span:
            scale = 1.0 / pivots[j][j]
            lines[j] = lines[j] * scale
            pivots[j] = [p * scale for p in pivots[j]]
            for i in span:
                if i != j:
                    factor = pivots[i][j]
                    lines[i] = lines[i] - factor * lines[j]
                    pivots[i] = [p - factor * q for p, q in zip(pivots[i], pivots[j])]
        update = columns[0] * lines[0]
        for j in span[1:]:
            update = update + columns[j] * lines[j]
        system = system - update
        for j in span:
            system = jnp.where(rows == k + j, lines[j], system)
    return system[:, size:]


def identity(size):
    return (
        lax.broadcasted_iota(jnp.int32, (size, size), 0)
        == lax.broadcasted_iota(jnp.int32, (size, size), 1)
    ).astype(jnp.float32)


def packed(gram, width):
    groups = max(1, width // gram.shape[1])
    depth = gram.shape[0] // groups
    return jnp.concatenate([gram[g * depth : (g + 1) * depth] for g in range(groups)], axis=1)


def unpacked(tile, size):
    groups = max(1, tile.shape[1] // size)
    return jnp.concatenate([tile[:, g * size : (g + 1) * size] for g in range(groups)], axis=0)


def kernel(
    extents,
    operator_hbm,
    load_hbm,
    modes_hbm,
    coarse_hbm,
    count_ref,
    maps_hbm,
    multipliers_ref,
    residual_ref,
    raw,
    load_ref,
    modes_ref,
    coarse_ref,
    maps_ref,
    ordered,
    own_modes,
    all_modes,
    padded_load,
    probes,
    first_out,
    first_in,
    pair_out,
    pair_in,
    face_out,
    face_in,
    last_out,
    last_in,
    load_in,
    plane_sums,
    line_sums,
    raw_sem,
    first_send,
    first_recv,
    face_send,
    face_recv,
    pair_send,
    pair_recv,
    last_send,
    last_recv,
    load_send,
    load_recv,
    plane_send,
    plane_recv,
    line_send,
    line_recv,
):
    nx, ny, nz = extents
    cases = load_hbm.shape[0]
    width = load_hbm.shape[1] // 3
    modes = modes_hbm.shape[0]
    padded = own_modes.shape[0]
    here = (lax.axis_index("gx"), lax.axis_index("gy"), lax.axis_index("gz"))
    ix, iy, iz = here
    plane = nx * ny
    slot = ix * ny + iy

    fetches = [
        pltpu.make_async_copy(source, target, raw_sem.at[i])
        for i, (source, target) in enumerate(
            (
                (maps_hbm, maps_ref),
                (modes_hbm, modes_ref),
                (coarse_hbm, coarse_ref),
                (load_hbm, load_ref),
                (operator_hbm, raw),
            )
        )
    ]
    for fetch in fetches:
        fetch.start()

    all_modes[...] = jnp.zeros(all_modes.shape, jnp.float32)
    probes[...] = jnp.zeros(probes.shape, jnp.float32)
    first_in[...] = jnp.zeros(first_in.shape, jnp.float32)
    pair_in[...] = jnp.zeros(pair_in.shape, jnp.float32)
    pair_out[...] = jnp.zeros(pair_out.shape, jnp.float32)
    face_out[:, :, cases:, :] = jnp.zeros((2, 6, 2 * padded, width), jnp.float32)
    face_in[:, :, cases:, :] = jnp.zeros((2, 6, 2 * padded, width), jnp.float32)
    own_modes[...] = jnp.zeros(own_modes.shape, jnp.float32)
    padded_load[...] = jnp.zeros(padded_load.shape, jnp.float32)

    def plane_peer(offset):
        other = lax.rem(slot + offset, plane)
        return (lax.div(other, ny), lax.rem(other, ny), iz)

    def line_peer(offset):
        return (ix, iy, lax.rem(iz + offset, nz))

    exists = []
    neighbour = []
    for d in range(3):
        exists.append(here[d] > 0)
        exists.append(here[d] < extents[d] - 1)
        for step in (-1, 1):
            neighbour.append(tuple(here[a] + (step if a == d else 0) for a in range(3)))
    flags = [jnp.where(e, 1, 0).astype(jnp.int32) for e in exists]

    def moved(position, f):
        return tuple(position[a] + ((2 * (f % 2) - 1) if a == f // 2 else 0) for a in range(3))

    def both_exist(f, g):
        if f != g:
            return jnp.logical_and(exists[f], exists[g])
        if f % 2:
            return here[f // 2] < extents[f // 2] - 2
        return here[f // 2] > 1

    pairs = [
        (f, g)
        for f in range(6)
        for g in range(6)
        if (f == g or f // 2 < g // 2) and extents[f // 2] > 1 + (f == g) and extents[g // 2] > 1
    ]

    barrier = pltpu.get_barrier_semaphore()
    diagonal = 0
    for f in range(4):
        for g in range(4, 6):
            peer = moved(moved(here, f), g)

            @pl.when(both_exist(f, g))
            def _(peer=peer):
                pl.semaphore_signal(barrier, inc=1, device_id=peer, device_id_type=MESH)

            diagonal = diagonal + flags[f] * flags[g]
    for offset in range(1, plane):
        pl.semaphore_signal(barrier, inc=1, device_id=plane_peer(offset), device_id_type=MESH)
    for offset in range(1, nz):
        pl.semaphore_signal(barrier, inc=1, device_id=line_peer(offset), device_id_type=MESH)


    def face(values, f):
        return values[:, f * width : (f + 1) * width]

    def masked(values, f):
        return jnp.where(jnp.full(values.shape, flags[f], jnp.int32) == 1, values, 0.0)

    sends = [[] for _ in range(6)]
    pair_sends = [[] for _ in pairs]

    def remote(source, target, send, recv, where):
        return pltpu.make_async_remote_copy(
            src_ref=source,
            dst_ref=target,
            send_sem=send,
            recv_sem=recv,
            device_id=where,
            device_id_type=MESH,
        )

    def start_to(f, copies):
        @pl.when(exists[f])
        def _():
            for copy in copies:
                copy.start()

        sends[f].extend(copies)

    for fetch in fetches[:4]:
        fetch.wait()
    count = count_ref[0, 0]
    lines = lax.broadcasted_iota(jnp.int32, (width, width), 0)
    orders = [(lines == maps_ref[d]).astype(jnp.float32) for d in range(3)]
    for m in range(modes):
        own_modes[m : m + 1, :] = modes_ref[m]
        padded_load[m : m + 1, 0:cases] = coarse_ref[m]
    raw_modes = jnp.where(
        lax.broadcasted_iota(jnp.int32, own_modes.shape, 0) < count, own_modes[...], 0.0
    )
    pieces = []
    for d in range(3):
        pieces.append(masked(mul(face(raw_modes, 2 * d), orders[d], NT), 2 * d))
        pieces.append(masked(face(raw_modes, 2 * d + 1), 2 * d + 1))
    mode_rows = jnp.concatenate(pieces, axis=1)
    own_modes[...] = mode_rows
    all_modes[0:padded, :] = mode_rows
    inactive = lax.broadcasted_iota(jnp.int32, (padded, padded), 0) >= count
    normal = mul(mode_rows, mode_rows, NT) + jnp.where(inactive, identity(padded), 0.0)
    coarse_inverse = eliminate(jnp.concatenate([normal, identity(padded)], axis=1), padded)
    active_load = jnp.where(
        lax.broadcasted_iota(jnp.int32, padded_load.shape, 0) < count, padded_load[...], 0.0
    )
    first_part = mul(coarse_inverse, active_load)
    inverse_modes = mul(coarse_inverse, mode_rows)
    probes[6 * padded :, :] = inverse_modes
    for f in range(6):
        first_out[f, 0:padded, :] = -face(mode_rows, f)
        first_out[f, padded : 2 * padded, :] = face(inverse_modes, f)
        first_out[f, 2 * padded :, :] = first_part

    pl.semaphore_wait(barrier, plane - 1 + nz - 1 + diagonal)

    for f in range(6):
        copies = [
            remote(first_out.at[f], first_in.at[f ^ 1], first_send.at[f], first_recv.at[f ^ 1], neighbour[f])
        ]
        if f % 2:
            d = f // 2
            copies.append(
                remote(
                    load_ref.at[:, pl.ds(d * width, width)],
                    load_in.at[d],
                    load_send.at[d],
                    load_recv.at[d],
                    neighbour[f],
                )
            )
        start_to(f, copies)

    def send_round(phase, values, own=None):
        found = fast(probes[...], values, NT)
        share = found[6 * padded :] if own is None else own - found[6 * padded :]
        for f in range(6):
            face_out[phase, f, 0:cases, :] = face(values, f)
            face_out[phase, f, cases : cases + padded, 0:cases] = share
            face_out[phase, f, cases + padded :, 0:cases] = found[f * padded : (f + 1) * padded]
        for index, (f, g) in enumerate(pairs):
            pair_out[phase, index, 0:padded, 0:cases] = found[f * padded : (f + 1) * padded]
            if f != g:
                pair_out[phase, index, padded:, 0:cases] = found[g * padded : (g + 1) * padded]
        for index, (f, g) in enumerate(pairs):
            other = pairs.index((f ^ 1, g ^ 1))
            copy = remote(
                pair_out.at[phase, index],
                pair_in.at[phase, other],
                pair_send.at[phase, index],
                pair_recv.at[phase, other],
                moved(moved(here, f), g),
            )
            pl.when(both_exist(f, g))(copy.start)
            pair_sends[index].append(copy)
        for f in range(6):
            start_to(
                f,
                [
                    remote(
                        face_out.at[phase, f],
                        face_in.at[phase, f ^ 1],
                        face_send.at[phase, f],
                        face_recv.at[phase, f ^ 1],
                        neighbour[f],
                    )
                ],
            )
        return found, share

    def wait_faces(phase, source, target, send, recv):
        for f in range(6):
            copy = remote(
                source.at[phase, f], target.at[phase, f], send.at[phase, f], recv.at[phase, f], neighbour[f]
            )
            pl.when(exists[f])(copy.wait_recv)

    def wait_pairs(phase):
        for index, (f, g) in enumerate(pairs):
            copy = remote(
                pair_out.at[phase, index],
                pair_in.at[phase, index],
                pair_send.at[phase, index],
                pair_recv.at[phase, index],
                moved(moved(here, f), g),
            )
            pl.when(both_exist(f, g))(copy.wait_recv)

    def assembled(mine, theirs, phase):
        return jnp.concatenate(
            [
                masked(mine[phase, f, 0:cases, :] - theirs[phase, f, 0:cases, :], f)
                for f in range(6)
            ],
            axis=1,
        )

    def apply_local(values):
        head = values.astype(jnp.bfloat16)
        tail = (values - head.astype(jnp.float32)).astype(jnp.bfloat16)
        both = jnp.dot(
            jnp.concatenate([head, tail], axis=0),
            ordered[...],
            preferred_element_type=jnp.float32,
        )
        return both[0:cases] + both[cases:]

    def owned(values):
        return jnp.concatenate([face(values, 1), face(values, 3), face(values, 5)], axis=1)

    fetches[4].wait()
    narrow = [order.astype(jnp.bfloat16) for order in orders]
    for d in range(3):
        low = 2 * d * width
        raw[pl.ds(low, width), :] = jnp.dot(
            narrow[d], raw[pl.ds(low, width), :], preferred_element_type=jnp.float32
        ).astype(jnp.bfloat16)
    for d in range(3):
        low = 2 * d * width
        ordered[:, low : low + width] = lax.dot_general(
            raw[:, low : low + width], narrow[d], NT, preferred_element_type=jnp.float32
        ).astype(jnp.bfloat16)
        ordered[:, low + width : low + 2 * width] = raw[:, low + width : low + 2 * width]
    for f in range(6):
        d = f // 2
        first = remote(first_out.at[f], first_in.at[f], first_send.at[f], first_recv.at[f], neighbour[f])
        pl.when(exists[f])(first.wait_recv)
    coefficients = [first_part]
    for f in range(6):
        all_modes[(1 + f) * padded : (2 + f) * padded, f * width : (f + 1) * width] = first_in[
            f, 0:padded, :
        ]
        probes[f * padded : (f + 1) * padded, f * width : (f + 1) * width] = first_in[
            f, padded : 2 * padded, :
        ]
        coefficients.append(first_in[f, 2 * padded :, :])
    initial = fast(jnp.concatenate(coefficients, axis=0)[:, 0:cases], all_modes[...], TN)
    product = apply_local(initial)
    right = []
    for d in range(3):
        copy = remote(
            load_ref.at[:, pl.ds(d * width, width)],
            load_in.at[d],
            load_send.at[d],
            load_recv.at[d],
            neighbour[2 * d],
        )
        pl.when(exists[2 * d])(copy.wait_recv)
    for d in range(3):
        right.append(masked(-load_in[d], 2 * d))
        right.append(masked(load_ref[:, d * width : (d + 1) * width], 2 * d + 1))
    right = jnp.concatenate(right, axis=1)
    shares = send_round(0, product, fast(inverse_modes, right, NT))
    wait_faces(0, face_out, face_in, face_send, face_recv)
    residual = right - assembled(face_out, face_in, 0)

    def preconditioned(phase, values, shares, sign):
        found, own = shares
        back = face_in[phase, 0, cases + padded :, 0:cases]
        for f in range(1, 6):
            back = back + face_in[phase, f, cases + padded :, 0:cases]
        own = own - sign * back
        wait_pairs(phase)
        terms = [found[f * padded : (f + 1) * padded] for f in range(6)]
        for index, (a, b) in enumerate(pairs):
            terms[b] = terms[b] + pair_in[phase, index, 0:padded, 0:cases]
            if a != b:
                terms[a] = terms[a] + pair_in[phase, index, padded:, 0:cases]
        every = [own]
        for f in range(6):
            every.append(face_in[phase, f, cases : cases + padded, 0:cases] - sign * terms[f])
        return values - 0.25 * fast(jnp.concatenate(every, axis=0), all_modes[...], TN)

    def sum_start(which, tile):
        plane_sums[which, slot] = tile
        copies = []
        for offset in range(1, plane):
            copy = remote(
                plane_sums.at[which, slot],
                plane_sums.at[which, slot],
                plane_send.at[which, offset],
                plane_recv.at[which, offset],
                plane_peer(offset),
            )
            copy.start()
            copies.append(copy)
        return copies

    def sum_middle(which, copies):
        for offset in range(1, plane):
            copy = remote(
                plane_sums.at[which, slot],
                plane_sums.at[which, lax.rem(slot + plane - offset, plane)],
                plane_send.at[which, offset],
                plane_recv.at[which, offset],
                plane_peer(offset),
            )
            copy.wait_recv()
        total = plane_sums[which, 0]
        for other in range(1, plane):
            total = total + plane_sums[which, other]
        line_sums[which, iz] = total
        for offset in range(1, nz):
            copy = remote(
                line_sums.at[which, iz],
                line_sums.at[which, iz],
                line_send.at[which, offset],
                line_recv.at[which, offset],
                line_peer(offset),
            )
            copy.start()
            copies.append(copy)

    def sum_end(which):
        for offset in range(1, nz):
            copy = remote(
                line_sums.at[which, iz],
                line_sums.at[which, lax.rem(iz + nz - offset, nz)],
                line_send.at[which, offset],
                line_recv.at[which, offset],
                line_peer(offset),
            )
            copy.wait_recv()
        total = line_sums[which, 0]
        for other in range(1, nz):
            total = total + line_sums[which, other]
        half = total.shape[0] // 2
        return unpacked(total[0:half], cases), unpacked(total[half:], cases)

    start = preconditioned(0, residual, shares, -1.0)
    product = apply_local(start)
    shares = send_round(1, product)
    early = sum_start(
        0,
        jnp.concatenate(
            [
                packed(fast(owned(start), owned(residual), NT), width),
                packed(fast(start, product, NT), width),
            ],
            axis=0,
        ),
    )
    wait_faces(1, face_out, face_in, face_send, face_recv)
    image = assembled(face_out, face_in, 1)
    sum_middle(0, early)
    second = preconditioned(1, image, shares, 1.0)
    product = apply_local(second)
    late = sum_start(
        1,
        jnp.concatenate(
            [
                packed(fast(owned(second), owned(image), NT), width),
                packed(fast(second, product, NT), width),
            ],
            axis=0,
        ),
    )
    for f in range(6):
        last_out[0, f] = face(product, f)
    for f in range(6):
        start_to(
            f,
            [
                remote(
                    last_out.at[0, f],
                    last_in.at[0, f ^ 1],
                    last_send.at[0, f],
                    last_recv.at[0, f ^ 1],
                    neighbour[f],
                )
            ],
        )
    gram, energy = sum_end(0)
    inverse = eliminate(jnp.concatenate([energy, identity(cases)], axis=1), cases)
    alpha = fast(inverse, gram)
    sum_middle(1, late)
    wait_faces(0, last_out, last_in, last_send, last_recv)
    second_image = assembled(last_out, last_in, 0)
    cross, last = sum_end(1)
    carried = fast(inverse, cross)
    schur = last - fast(cross, carried)
    right_side = fast(cross, alpha) - energy
    tail = eliminate(jnp.concatenate([schur, right_side], axis=1), cases)
    head = alpha + fast(carried, tail)
    both = jnp.concatenate([head, -tail], axis=0)
    multipliers_ref[...] = owned(initial) + fast(
        both, jnp.concatenate([owned(start), owned(second)], axis=0), TN
    )
    residual_ref[...] = owned(residual) - fast(
        both, jnp.concatenate([owned(image), owned(second_image)], axis=0), TN
    )

    def finish(condition, copies):
        @pl.when(condition)
        def _():
            for copy in copies:
                copy.wait_send()

    for f in range(6):
        finish(exists[f], sends[f])
    for index, (f, g) in enumerate(pairs):
        finish(both_exist(f, g), pair_sends[index])
    for copy in early + late:
        copy.wait_send()


def held(array):
    return pltpu.with_memory_space_constraint(array, pltpu.HBM)


def rows_apart(array):
    return jnp.swapaxes(array, 2, 3).reshape(array.shape[3], 1, array.shape[4])


def local(extents, dual_operators, dual_load, rigid_modes, coarse_load, mode_counts, face_maps):
    size = dual_operators.shape[-1]
    cases = dual_load.shape[-2]
    width = dual_load.shape[-1] // 3
    modes = rigid_modes.shape[-2]
    padded = -(-modes // 8) * 8
    nx, ny, nz = extents
    plane = nx * ny
    tile = 2 * cases // max(1, width // cases)
    f32 = jnp.float32
    vmem = pl.BlockSpec(memory_space=pltpu.VMEM)
    hbm = pl.BlockSpec(memory_space=pltpu.HBM)
    dma = pltpu.SemaphoreType.DMA
    out = jax.ShapeDtypeStruct((cases, 3 * width), f32)
    multipliers, residual = pl.pallas_call(
        functools.partial(kernel, extents),
        out_shape=(out, out),
        in_specs=[
            hbm,
            hbm,
            hbm,
            hbm,
            pl.BlockSpec(memory_space=pltpu.SMEM),
            hbm,
        ],
        out_specs=(vmem, vmem),
        scratch_shapes=[
            pltpu.VMEM((size, size), dual_operators.dtype),
            pltpu.VMEM((cases, 3 * width), f32),
            pltpu.VMEM((modes, 1, size), f32),
            pltpu.VMEM((modes, 1, cases), f32),
            pltpu.VMEM((3, 1, width), jnp.int32),
            pltpu.VMEM((size, size), dual_operators.dtype),
            pltpu.VMEM((padded, size), f32),
            pltpu.VMEM((7 * padded, size), f32),
            pltpu.VMEM((padded, width), f32),
            pltpu.VMEM((7 * padded, size), f32),
            pltpu.VMEM((6, 3 * padded, width), f32),
            pltpu.VMEM((6, 3 * padded, width), f32),
            pltpu.VMEM((2, 18, 2 * padded, width), f32),
            pltpu.VMEM((2, 18, 2 * padded, width), f32),
            pltpu.VMEM((2, 6, cases + 2 * padded, width), f32),
            pltpu.VMEM((2, 6, cases + 2 * padded, width), f32),
            pltpu.VMEM((1, 6, cases, width), f32),
            pltpu.VMEM((1, 6, cases, width), f32),
            pltpu.VMEM((3, cases, width), f32),
            pltpu.VMEM((2, plane, tile, width), f32),
            pltpu.VMEM((2, nz, tile, width), f32),
            dma((5,)),
            dma((6,)),
            dma((6,)),
            dma((2, 6)),
            dma((2, 6)),
            dma((2, 18)),
            dma((2, 18)),
            dma((1, 6)),
            dma((1, 6)),
            dma((3,)),
            dma((3,)),
            dma((2, plane)),
            dma((2, plane)),
            dma((2, nz)),
            dma((2, nz)),
        ],
        compiler_params=pltpu.CompilerParams(collective_id=0, has_side_effects=True, vmem_limit_bytes=16 * 1024 * 1024
        ),
    )(
        held(dual_operators.reshape(size, size)),
        held(dual_load.reshape(cases, 3 * width)),
        held(rows_apart(rigid_modes)),
        held(rows_apart(coarse_load)),
        mode_counts.reshape(1, 1),
        held(rows_apart(face_maps)),
    )
    shape = (1, 1, 1, cases, 3 * width)
    return multipliers.reshape(shape), residual.reshape(shape)


def solution(mesh):
    extents = (mesh.shape["gx"], mesh.shape["gy"], mesh.shape["gz"])
    spec = P("gx", "gy", "gz", None, None)
    return jax.shard_map(
        functools.partial(local, extents),
        mesh=mesh,
        in_specs=(spec, spec, spec, spec, P("gx", "gy", "gz"), spec),
        out_specs=(spec, spec),
        check_vma=False,
    )
```

```python
import functools

import jax
import jax.numpy as jnp
from jax import lax
from jax.experimental import pallas as pl
from jax.experimental.pallas import tpu as pltpu
from jax.sharding import PartitionSpec as P

MESH = pl.DeviceIdType.MESH
HIGH = lax.Precision.HIGHEST
NN = (((1,), (0,)), ((), ()))
NT = (((1,), (1,)), ((), ()))
TN = (((0,), (0,)), ((), ()))


def mul(a, b, dims=NN):
    return lax.dot_general(a, b, dims, precision=HIGH, preferred_element_type=jnp.float32)


def split(a):
    head = a.astype(jnp.bfloat16)
    return head, (a - head.astype(jnp.float32)).astype(jnp.bfloat16)


def fast(a, b, dims=NN):
    if dims == TN:
        a, dims = a.T, NN
    (ah, al), (bh, bl) = split(a), split(b)
    dot = functools.partial(
        lax.dot_general, dimension_numbers=dims, preferred_element_type=jnp.float32
    )
    return dot(ah, bh) + (dot(ah, bl) + dot(al, bh))


def eliminate(system, size, block=8):
    rows = lax.broadcasted_iota(jnp.int32, system.shape, 0)
    span = range(block)
    for k in range(0, size, block):
        columns = [system[:, k + j : k + j + 1] for j in span]
        lines = [system[k + i : k + i + 1, :] for i in span]
        pivots = [
            [jnp.broadcast_to(lines[i][:, k + j : k + j + 1], lines[i].shape) for j in span]
            for i in span
        ]
        for j in span:
            scale = 1.0 / pivots[j][j]
            lines[j] = lines[j] * scale
            pivots[j] = [p * scale for p in pivots[j]]
            for i in span:
                if i != j:
                    factor = pivots[i][j]
                    lines[i] = lines[i] - factor * lines[j]
                    pivots[i] = [p - factor * q for p, q in zip(pivots[i], pivots[j])]
        update = columns[0] * lines[0]
        for j in span[1:]:
            update = update + columns[j] * lines[j]
        system = system - update
        for j in span:
            system = jnp.where(rows == k + j, lines[j], system)
    return system[:, size:]


def identity(size):
    return (
        lax.broadcasted_iota(jnp.int32, (size, size), 0)
        == lax.broadcasted_iota(jnp.int32, (size, size), 1)
    ).astype(jnp.float32)


def packed(gram, width):
    groups = max(1, width // gram.shape[1])
    depth = gram.shape[0] // groups
    return jnp.concatenate([gram[g * depth : (g + 1) * depth] for g in range(groups)], axis=1)


def unpacked(tile, size):
    groups = max(1, tile.shape[1] // size)
    return jnp.concatenate([tile[:, g * size : (g + 1) * size] for g in range(groups)], axis=0)


def kernel(
    extents,
    operator_hbm,
    load_hbm,
    modes_hbm,
    coarse_hbm,
    count_ref,
    maps_hbm,
    multipliers_ref,
    residual_ref,
    raw,
    load_ref,
    modes_ref,
    coarse_ref,
    maps_ref,
    ordered,
    own_modes,
    all_modes,
    padded_load,
    probes,
    first_out,
    first_in,
    pair_out,
    pair_in,
    face_out,
    face_in,
    last_out,
    last_in,
    load_in,
    plane_sums,
    line_sums,
    raw_sem,
    first_send,
    first_recv,
    face_send,
    face_recv,
    pair_send,
    pair_recv,
    last_send,
    last_recv,
    load_send,
    load_recv,
    plane_send,
    plane_recv,
    line_send,
    line_recv,
):
    nx, ny, nz = extents
    cases = load_hbm.shape[0]
    width = load_hbm.shape[1] // 3
    modes = modes_hbm.shape[0]
    padded = own_modes.shape[0]
    here = (lax.axis_index("gx"), lax.axis_index("gy"), lax.axis_index("gz"))
    ix, iy, iz = here
    plane = nx * ny
    slot = ix * ny + iy

    fetches = [
        pltpu.make_async_copy(source, target, raw_sem.at[i])
        for i, (source, target) in enumerate(
            (
                (maps_hbm, maps_ref),
                (modes_hbm, modes_ref),
                (coarse_hbm, coarse_ref),
                (load_hbm, load_ref),
                (operator_hbm, raw),
            )
        )
    ]
    for fetch in fetches:
        fetch.start()

    all_modes[...] = jnp.zeros(all_modes.shape, jnp.float32)
    probes[...] = jnp.zeros(probes.shape, jnp.float32)
    first_in[...] = jnp.zeros(first_in.shape, jnp.float32)
    pair_in[...] = jnp.zeros(pair_in.shape, jnp.float32)
    pair_out[...] = jnp.zeros(pair_out.shape, jnp.float32)
    face_out[:, :, cases:, :] = jnp.zeros((2, 6, 2 * padded, width), jnp.float32)
    face_in[:, :, cases:, :] = jnp.zeros((2, 6, 2 * padded, width), jnp.float32)
    own_modes[...] = jnp.zeros(own_modes.shape, jnp.float32)
    padded_load[...] = jnp.zeros(padded_load.shape, jnp.float32)

    def plane_peer(offset):
        other = lax.rem(slot + offset, plane)
        return (lax.div(other, ny), lax.rem(other, ny), iz)

    def line_peer(offset):
        return (ix, iy, lax.rem(iz + offset, nz))

    exists = []
    neighbour = []
    for d in range(3):
        exists.append(here[d] > 0)
        exists.append(here[d] < extents[d] - 1)
        for step in (-1, 1):
            neighbour.append(tuple(here[a] + (step if a == d else 0) for a in range(3)))
    flags = [jnp.where(e, 1, 0).astype(jnp.int32) for e in exists]

    def moved(position, f):
        return tuple(position[a] + ((2 * (f % 2) - 1) if a == f // 2 else 0) for a in range(3))

    def both_exist(f, g):
        if f != g:
            return jnp.logical_and(exists[f], exists[g])
        if f % 2:
            return here[f // 2] < extents[f // 2] - 2
        return here[f // 2] > 1

    pairs = [
        (f, g)
        for f in range(6)
        for g in range(6)
        if (f == g or f // 2 < g // 2) and extents[f // 2] > 1 + (f == g) and extents[g // 2] > 1
    ]

    barrier = pltpu.get_barrier_semaphore()
    diagonal = 0
    for f in range(4):
        for g in range(4, 6):
            peer = moved(moved(here, f), g)

            @pl.when(both_exist(f, g))
            def _(peer=peer):
                pl.semaphore_signal(barrier, inc=1, device_id=peer, device_id_type=MESH)

            diagonal = diagonal + flags[f] * flags[g]
    for offset in range(1, plane):
        pl.semaphore_signal(barrier, inc=1, device_id=plane_peer(offset), device_id_type=MESH)
    for offset in range(1, nz):
        pl.semaphore_signal(barrier, inc=1, device_id=line_peer(offset), device_id_type=MESH)


    def face(values, f):
        return values[:, f * width : (f + 1) * width]

    def masked(values, f):
        return jnp.where(jnp.full(values.shape, flags[f], jnp.int32) == 1, values, 0.0)

    sends = [[] for _ in range(6)]
    pair_sends = [[] for _ in pairs]

    def remote(source, target, send, recv, where):
        return pltpu.make_async_remote_copy(
            src_ref=source,
            dst_ref=target,
            send_sem=send,
            recv_sem=recv,
            device_id=where,
            device_id_type=MESH,
        )

    def start_to(f, copies):
        @pl.when(exists[f])
        def _():
            for copy in copies:
                copy.start()

        sends[f].extend(copies)

    for fetch in fetches[:4]:
        fetch.wait()
    count = count_ref[0, 0]
    lines = lax.broadcasted_iota(jnp.int32, (width, width), 0)
    orders = [(lines == maps_ref[d]).astype(jnp.float32) for d in range(3)]
    for m in range(modes):
        own_modes[m : m + 1, :] = modes_ref[m]
        padded_load[m : m + 1, 0:cases] = coarse_ref[m]
    raw_modes = jnp.where(
        lax.broadcasted_iota(jnp.int32, own_modes.shape, 0) < count, own_modes[...], 0.0
    )
    pieces = []
    for d in range(3):
        pieces.append(masked(mul(face(raw_modes, 2 * d), orders[d], NT), 2 * d))
        pieces.append(masked(face(raw_modes, 2 * d + 1), 2 * d + 1))
    mode_rows = jnp.concatenate(pieces, axis=1)
    own_modes[...] = mode_rows
    all_modes[0:padded, :] = mode_rows
    inactive = lax.broadcasted_iota(jnp.int32, (padded, padded), 0) >= count
    normal = mul(mode_rows, mode_rows, NT) + jnp.where(inactive, identity(padded), 0.0)
    coarse_inverse = eliminate(jnp.concatenate([normal, identity(padded)], axis=1), padded)
    active_load = jnp.where(
        lax.broadcasted_iota(jnp.int32, padded_load.shape, 0) < count, padded_load[...], 0.0
    )
    first_part = mul(coarse_inverse, active_load)
    inverse_modes = mul(coarse_inverse, mode_rows)
    probes[6 * padded :, :] = inverse_modes
    for f in range(6):
        first_out[f, 0:padded, :] = -face(mode_rows, f)
        first_out[f, padded : 2 * padded, :] = face(inverse_modes, f)
        first_out[f, 2 * padded :, :] = first_part

    pl.semaphore_wait(barrier, plane - 1 + nz - 1 + diagonal)

    for f in range(6):
        copies = [
            remote(first_out.at[f], first_in.at[f ^ 1], first_send.at[f], first_recv.at[f ^ 1], neighbour[f])
        ]
        if f % 2:
            d = f // 2
            copies.append(
                remote(
                    load_ref.at[:, pl.ds(d * width, width)],
                    load_in.at[d],
                    load_send.at[d],
                    load_recv.at[d],
                    neighbour[f],
                )
            )
        start_to(f, copies)

    def send_round(phase, values, own=None):
        found = fast(probes[...], values, NT)
        share = found[6 * padded :] if own is None else own - found[6 * padded :]
        for f in range(6):
            face_out[phase, f, 0:cases, :] = face(values, f)
            face_out[phase, f, cases : cases + padded, 0:cases] = share
            face_out[phase, f, cases + padded :, 0:cases] = found[f * padded : (f + 1) * padded]
        for index, (f, g) in enumerate(pairs):
            pair_out[phase, index, 0:padded, 0:cases] = found[f * padded : (f + 1) * padded]
            if f != g:
                pair_out[phase, index, padded:, 0:cases] = found[g * padded : (g + 1) * padded]
        for index, (f, g) in enumerate(pairs):
            other = pairs.index((f ^ 1, g ^ 1))
            copy = remote(
                pair_out.at[phase, index],
                pair_in.at[phase, other],
                pair_send.at[phase, index],
                pair_recv.at[phase, other],
                moved(moved(here, f), g),
            )
            pl.when(both_exist(f, g))(copy.start)
            pair_sends[index].append(copy)
        for f in range(6):
            start_to(
                f,
                [
                    remote(
                        face_out.at[phase, f],
                        face_in.at[phase, f ^ 1],
                        face_send.at[phase, f],
                        face_recv.at[phase, f ^ 1],
                        neighbour[f],
                    )
                ],
            )
        return found, share

    def wait_faces(phase, source, target, send, recv):
        for f in range(6):
            copy = remote(
                source.at[phase, f], target.at[phase, f], send.at[phase, f], recv.at[phase, f], neighbour[f]
            )
            pl.when(exists[f])(copy.wait_recv)

    def wait_pairs(phase):
        for index, (f, g) in enumerate(pairs):
            copy = remote(
                pair_out.at[phase, index],
                pair_in.at[phase, index],
                pair_send.at[phase, index],
                pair_recv.at[phase, index],
                moved(moved(here, f), g),
            )
            pl.when(both_exist(f, g))(copy.wait_recv)

    def assembled(mine, theirs, phase):
        return jnp.concatenate(
            [
                masked(mine[phase, f, 0:cases, :] - theirs[phase, f, 0:cases, :], f)
                for f in range(6)
            ],
            axis=1,
        )

    def apply_local(values):
        head = values.astype(jnp.bfloat16)
        tail = (values - head.astype(jnp.float32)).astype(jnp.bfloat16)
        both = jnp.dot(
            jnp.concatenate([head, tail], axis=0),
            ordered[...],
            preferred_element_type=jnp.float32,
        )
        return both[0:cases] + both[cases:]

    def owned(values):
        return jnp.concatenate([face(values, 1), face(values, 3), face(values, 5)], axis=1)

    fetches[4].wait()
    narrow = [order.astype(jnp.bfloat16) for order in orders]
    for d in range(3):
        low = 2 * d * width
        raw[pl.ds(low, width), :] = jnp.dot(
            narrow[d], raw[pl.ds(low, width), :], preferred_element_type=jnp.float32
        ).astype(jnp.bfloat16)
    for d in range(3):
        low = 2 * d * width
        ordered[:, low : low + width] = lax.dot_general(
            raw[:, low : low + width], narrow[d], NT, preferred_element_type=jnp.float32
        ).astype(jnp.bfloat16)
        ordered[:, low + width : low + 2 * width] = raw[:, low + width : low + 2 * width]
    for f in range(6):
        d = f // 2
        first = remote(first_out.at[f], first_in.at[f], first_send.at[f], first_recv.at[f], neighbour[f])
        pl.when(exists[f])(first.wait_recv)
    coefficients = [first_part]
    for f in range(6):
        all_modes[(1 + f) * padded : (2 + f) * padded, f * width : (f + 1) * width] = first_in[
            f, 0:padded, :
        ]
        probes[f * padded : (f + 1) * padded, f * width : (f + 1) * width] = first_in[
            f, padded : 2 * padded, :
        ]
        coefficients.append(first_in[f, 2 * padded :, :])
    initial = fast(jnp.concatenate(coefficients, axis=0)[:, 0:cases], all_modes[...], TN)
    product = apply_local(initial)
    right = []
    for d in range(3):
        copy = remote(
            load_ref.at[:, pl.ds(d * width, width)],
            load_in.at[d],
            load_send.at[d],
            load_recv.at[d],
            neighbour[2 * d],
        )
        pl.when(exists[2 * d])(copy.wait_recv)
    for d in range(3):
        right.append(masked(-load_in[d], 2 * d))
        right.append(masked(load_ref[:, d * width : (d + 1) * width], 2 * d + 1))
    right = jnp.concatenate(right, axis=1)
    shares = send_round(0, product, fast(inverse_modes, right, NT))
    wait_faces(0, face_out, face_in, face_send, face_recv)
    residual = right - assembled(face_out, face_in, 0)

    def preconditioned(phase, values, shares, sign):
        found, own = shares
        back = face_in[phase, 0, cases + padded :, 0:cases]
        for f in range(1, 6):
            back = back + face_in[phase, f, cases + padded :, 0:cases]
        own = own - sign * back
        wait_pairs(phase)
        terms = [found[f * padded : (f + 1) * padded] for f in range(6)]
        for index, (a, b) in enumerate(pairs):
            terms[b] = terms[b] + pair_in[phase, index, 0:padded, 0:cases]
            if a != b:
                terms[a] = terms[a] + pair_in[phase, index, padded:, 0:cases]
        every = [own]
        for f in range(6):
            every.append(face_in[phase, f, cases : cases + padded, 0:cases] - sign * terms[f])
        return values - 0.25 * fast(jnp.concatenate(every, axis=0), all_modes[...], TN)

    def sum_start(which, tile):
        plane_sums[which, slot] = tile
        copies = []
        for offset in range(1, plane):
            copy = remote(
                plane_sums.at[which, slot],
                plane_sums.at[which, slot],
                plane_send.at[which, offset],
                plane_recv.at[which, offset],
                plane_peer(offset),
            )
            copy.start()
            copies.append(copy)
        return copies

    def sum_middle(which, copies):
        for offset in range(1, plane):
            copy = remote(
                plane_sums.at[which, slot],
                plane_sums.at[which, lax.rem(slot + plane - offset, plane)],
                plane_send.at[which, offset],
                plane_recv.at[which, offset],
                plane_peer(offset),
            )
            copy.wait_recv()
        total = plane_sums[which, 0]
        for other in range(1, plane):
            total = total + plane_sums[which, other]
        line_sums[which, iz] = total
        for offset in range(1, nz):
            copy = remote(
                line_sums.at[which, iz],
                line_sums.at[which, iz],
                line_send.at[which, offset],
                line_recv.at[which, offset],
                line_peer(offset),
            )
            copy.start()
            copies.append(copy)

    def sum_end(which):
        for offset in range(1, nz):
            copy = remote(
                line_sums.at[which, iz],
                line_sums.at[which, lax.rem(iz + nz - offset, nz)],
                line_send.at[which, offset],
                line_recv.at[which, offset],
                line_peer(offset),
            )
            copy.wait_recv()
        total = line_sums[which, 0]
        for other in range(1, nz):
            total = total + line_sums[which, other]
        half = total.shape[0] // 2
        return unpacked(total[0:half], cases), unpacked(total[half:], cases)

    start = preconditioned(0, residual, shares, -1.0)
    product = apply_local(start)
    shares = send_round(1, product)
    early = sum_start(
        0,
        jnp.concatenate(
            [
                packed(fast(owned(start), owned(residual), NT), width),
                packed(fast(start, product, NT), width),
            ],
            axis=0,
        ),
    )
    wait_faces(1, face_out, face_in, face_send, face_recv)
    image = assembled(face_out, face_in, 1)
    sum_middle(0, early)
    second = preconditioned(1, image, shares, 1.0)
    product = apply_local(second)
    late = sum_start(
        1,
        jnp.concatenate(
            [
                packed(fast(owned(second), owned(image), NT), width),
                packed(fast(second, product, NT), width),
            ],
            axis=0,
        ),
    )
    for f in range(6):
        last_out[0, f] = face(product, f)
    for f in range(6):
        start_to(
            f,
            [
                remote(
                    last_out.at[0, f],
                    last_in.at[0, f ^ 1],
                    last_send.at[0, f],
                    last_recv.at[0, f ^ 1],
                    neighbour[f],
                )
            ],
        )
    gram, energy = sum_end(0)
    inverse = eliminate(jnp.concatenate([energy, identity(cases)], axis=1), cases)
    alpha = fast(inverse, gram)
    sum_middle(1, late)
    wait_faces(0, last_out, last_in, last_send, last_recv)
    second_image = assembled(last_out, last_in, 0)
    cross, last = sum_end(1)
    carried = fast(inverse, cross)
    schur = last - fast(cross, carried)
    right_side = fast(cross, alpha) - energy
    tail = eliminate(jnp.concatenate([schur, right_side], axis=1), cases)
    head = alpha + fast(carried, tail)
    both = jnp.concatenate([head, -tail], axis=0)
    multipliers_ref[...] = owned(initial) + fast(
        both, jnp.concatenate([owned(start), owned(second)], axis=0), TN
    )
    residual_ref[...] = owned(residual) - fast(
        both, jnp.concatenate([owned(image), owned(second_image)], axis=0), TN
    )

    def finish(condition, copies):
        @pl.when(condition)
        def _():
            for copy in copies:
                copy.wait_send()

    for f in range(6):
        finish(exists[f], sends[f])
    for index, (f, g) in enumerate(pairs):
        finish(both_exist(f, g), pair_sends[index])
    for copy in early + late:
        copy.wait_send()


def held(array):
    return pltpu.with_memory_space_constraint(array, pltpu.HBM)


def rows_apart(array):
    return jnp.swapaxes(array, 2, 3).reshape(array.shape[3], 1, array.shape[4])


def local(extents, dual_operators, dual_load, rigid_modes, coarse_load, mode_counts, face_maps):
    size = dual_operators.shape[-1]
    cases = dual_load.shape[-2]
    width = dual_load.shape[-1] // 3
    modes = rigid_modes.shape[-2]
    padded = -(-modes // 8) * 8
    nx, ny, nz = extents
    plane = nx * ny
    tile = 2 * cases // max(1, width // cases)
    f32 = jnp.float32
    vmem = pl.BlockSpec(memory_space=pltpu.VMEM)
    hbm = pl.BlockSpec(memory_space=pltpu.HBM)
    dma = pltpu.SemaphoreType.DMA
    out = jax.ShapeDtypeStruct((cases, 3 * width), f32)
    multipliers, residual = pl.pallas_call(
        functools.partial(kernel, extents),
        out_shape=(out, out),
        in_specs=[
            hbm,
            hbm,
            hbm,
            hbm,
            pl.BlockSpec(memory_space=pltpu.SMEM),
            hbm,
        ],
        out_specs=(vmem, vmem),
        scratch_shapes=[
            pltpu.VMEM((size, size), dual_operators.dtype),
            pltpu.VMEM((cases, 3 * width), f32),
            pltpu.VMEM((modes, 1, size), f32),
            pltpu.VMEM((modes, 1, cases), f32),
            pltpu.VMEM((3, 1, width), jnp.int32),
            pltpu.VMEM((size, size), dual_operators.dtype),
            pltpu.VMEM((padded, size), f32),
            pltpu.VMEM((7 * padded, size), f32),
            pltpu.VMEM((padded, width), f32),
            pltpu.VMEM((7 * padded, size), f32),
            pltpu.VMEM((6, 3 * padded, width), f32),
            pltpu.VMEM((6, 3 * padded, width), f32),
            pltpu.VMEM((2, 18, 2 * padded, width), f32),
            pltpu.VMEM((2, 18, 2 * padded, width), f32),
            pltpu.VMEM((2, 6, cases + 2 * padded, width), f32),
            pltpu.VMEM((2, 6, cases + 2 * padded, width), f32),
            pltpu.VMEM((1, 6, cases, width), f32),
            pltpu.VMEM((1, 6, cases, width), f32),
            pltpu.VMEM((3, cases, width), f32),
            pltpu.VMEM((2, plane, tile, width), f32),
            pltpu.VMEM((2, nz, tile, width), f32),
            dma((5,)),
            dma((6,)),
            dma((6,)),
            dma((2, 6)),
            dma((2, 6)),
            dma((2, 18)),
            dma((2, 18)),
            dma((1, 6)),
            dma((1, 6)),
            dma((3,)),
            dma((3,)),
            dma((2, plane)),
            dma((2, plane)),
            dma((2, nz)),
            dma((2, nz)),
        ],
        compiler_params=pltpu.CompilerParams(collective_id=0, has_side_effects=True, vmem_limit_bytes=16 * 1024 * 1024
        ),
    )(
        held(dual_operators.reshape(size, size)),
        held(dual_load.reshape(cases, 3 * width)),
        held(rows_apart(rigid_modes)),
        held(rows_apart(coarse_load)),
        mode_counts.reshape(1, 1),
        held(rows_apart(face_maps)),
    )
    shape = (1, 1, 1, cases, 3 * width)
    return multipliers.reshape(shape), residual.reshape(shape)


def solution(mesh):
    extents = (mesh.shape["gx"], mesh.shape["gy"], mesh.shape["gz"])
    spec = P("gx", "gy", "gz", None, None)
    return jax.shard_map(
        functools.partial(local, extents),
        mesh=mesh,
        in_specs=(spec, spec, spec, spec, P("gx", "gy", "gz"), spec),
        out_specs=(spec, spec),
        check_vma=False,
    )
```
